128 devices in a mesh: member: 8 (over x, y_lo), slab: 16 (over y_hi, z, core).
Axes of the slice: x: 4, y: 4 (y_hi: 2, y_lo: 2; y = y_hi * 2 + y_lo), z: 4, core: 2. Of those that a mesh axis runs over, the one named last changes fastest.
Arguments:
- control: float32 [32, 2, 1024, 2048], P('member', None, 'slab'), may hold values from -6 to 6
- perturbation: bfloat16 [32, 2, 1024, 2048], P('member', None, 'slab'), may hold values from -6 to 6
- loc_row: float32 [2, 1024], P(None, 'slab'), may hold values from 0.2 to 2
- loc_col: float32 [2, 2048], replicated, may hold values from 0.2 to 2
- obs_tile: int32 [4096], P('slab'), may hold values from 0 to 2047, as said below
- obs_count: int32 [4096], P('slab'), may hold values from 1 to 128
- obs_value: float32 [4096, 128], P('slab'), may hold values from -12 to 12
Outputs:
- gradient: float32 [32, 2, 1024, 2048], P('member', None, 'slab')
The draws below stay inside these ranges and needn't reach their ends.
Inputs may be any that keep to these rules, and one draw needn't show every extreme that they name: `obs_tile`: entry i names a tile of slab block i // 256 in that block's numbering, whose columns lie in column share k = (i mod 256) // (256 / 16), i.e. columns k * 2048 / 16 onward; tiles may repeat. cells 0 to obs_count - 1 of a tile are observed.
All inputs are finite; a program needn't handle non-finite values.
Results may differ from the reference program's by a relative error of at most 0.012.
Values may be sent and summed in bfloat16 or wider, within the bound.
No kernel may reach another device: no remote copies, remote signals or barrier semaphores. Data moves between devices by JAX's collectives and lax.ppermute only.
A program may use at most 64 MiB of HBM per device.

```python
import math
import jax
import jax.numpy as jnp
from jax import lax

NY = 1024
NX = 2048
LEV = 2
TILE = 128
OBS_DEV = 256
MEMBERS = 32
OBS = 4096
TILES_DEV = 2048
N_SLAB = 16


def draw_obs_tile(key, part):
    rows = NY // N_SLAB
    per_row = NX // TILE
    per_share = NX // N_SLAB // TILE
    index = jnp.arange(OBS, dtype=jnp.int32)
    share = index % OBS_DEV // (OBS_DEV // N_SLAB)
    key_level = jax.random.fold_in(key, 11)
    key_row = jax.random.fold_in(key, 23)
    key_within = jax.random.fold_in(key, 37)
    level = jax.random.randint(key_level, (OBS,), 0, LEV, dtype=jnp.int32)
    row_in = jax.random.randint(key_row, (OBS,), 0, rows, dtype=jnp.int32)
    within = jax.random.randint(key_within, (OBS,), 0, per_share, dtype=jnp.int32)
    column_tile = share * per_share + within
    return ((level * rows + row_in) * per_row + column_tile).astype(jnp.int32)


def touch_ends(values, stream_key, smallest, top_value):
    place = [jax.random.randint(jax.random.fold_in(stream_key, axis), (), 0, length) for axis, length in enumerate(values.shape)]
    longest = values.shape.index(max(values.shape))
    next_to = place[:longest] + [(place[longest] + 1) % values.shape[longest]] + place[longest + 1:]
    return values.at[tuple(place)].set(smallest).at[tuple(next_to)].set(top_value)


def block_levels(rng, extent, split, low, top_value):
    gain = 1.0
    for dim, blocks in split:
        heights = jax.random.uniform(jax.random.fold_in(jax.random.fold_in(rng, 6), dim), (blocks,), jnp.float32, low / len(split), top_value / len(split))
        gain = gain * jnp.repeat(jnp.exp(heights), extent[dim] // blocks).reshape((-1,) + (1,) * (len(extent) - 1 - dim))
    return gain


def scatter_about(own_key, extent, scale, bound, split=(), kind=jnp.bfloat16):
    array = scale * jax.random.normal(own_key, extent, jnp.float32)
    if split:
        array = array * block_levels(own_key, extent, split, -0.22, 0.18)
    return jnp.clip(array, -bound, bound).astype(kind)


def setup_inputs(seed: int = 0) -> dict:
    seeds = jax.random.split(jax.random.key(seed), 8)
    control = scatter_about(seeds[0], (MEMBERS, LEV, NY, NX), 1.0, 6.0, ((0, 8), (2, 16)), jnp.float32)
    perturbation = scatter_about(seeds[1], (MEMBERS, LEV, NY, NX), 1.0, 6.0, ((0, 8), (2, 16)))
    loc_row = jnp.clip(jnp.exp(math.log(2.0) - 2.3025851 * jax.random.uniform(seeds[2], (LEV, NY), jnp.float32) ** block_levels(seeds[2], (LEV, NY), ((1, 16),), -0.2, 0.2)), 0.2, 2.0)
    loc_col = jnp.clip(jnp.exp(jax.random.uniform(seeds[3], (LEV, NX), jnp.float32, math.log(0.2), math.log(2.0))), 0.2, 2.0)
    obs_tile = draw_obs_tile(jax.random.fold_in(seeds[7], 71), 0)
    obs_count = touch_ends(jax.random.randint(seeds[5], (OBS,), 1, TILE + 1), jax.random.fold_in(seeds[5], 1), 1, TILE).astype(jnp.int32)
    obs_value = scatter_about(seeds[6], (OBS, TILE), 2.0, 12.0, ((0, 16),), jnp.float32)
    return dict(control=control, perturbation=perturbation, loc_row=loc_row, loc_col=loc_col, obs_tile=obs_tile, obs_count=obs_count, obs_value=obs_value)


def hartley(order):
    index = jnp.arange(order, dtype=jnp.int32)
    product = index[:, None] * index[None, :] % order
    angle = 2.0 * jnp.pi * product.astype(jnp.float32) / order
    table = (jnp.cos(angle) + jnp.sin(angle)) / jnp.sqrt(jnp.float32(order))
    return table.astype(jnp.bfloat16).astype(jnp.float32)

def rounded(value):
    return lax.optimization_barrier(value.astype(jnp.bfloat16)).astype(jnp.float32)

def reference(control, perturbation, loc_row, loc_col, obs_tile, obs_count, obs_value):
    table_y = hartley(NY)
    table_x = hartley(NX)
    amplitude = loc_row[:, :, None] * loc_col[:, None, :]

    def forward(carry, pair):
        coeffs, member_pert = pair
        scaled = rounded(coeffs * amplitude)
        along = rounded(jnp.einsum('lab,bx->lax', scaled, table_x))
        field = rounded(jnp.einsum('ya,lax->lyx', table_y, along))
        return (carry + member_pert.astype(jnp.float32) * field, None)
    start = jnp.zeros((LEV, NY, NX), jnp.float32)
    increment, _ = lax.scan(forward, start, (control, perturbation))
    rows = NY // N_SLAB
    tiled = increment.reshape(LEV, N_SLAB, rows, NX // TILE, TILE)
    tiled = jnp.transpose(tiled, (1, 0, 2, 3, 4)).reshape(N_SLAB, TILES_DEV, TILE)
    block = (jnp.arange(OBS, dtype=jnp.int32) // OBS_DEV).astype(jnp.int32)
    cells = tiled[block, obs_tile]
    resid = cells - obs_value
    observed = jnp.arange(TILE, dtype=jnp.int32)[None, :] < obs_count[:, None]
    score = jnp.where(observed, resid / jnp.sqrt(1.0 + resid * resid / 4.0), 0.0)
    spread = jnp.zeros((N_SLAB, TILES_DEV, TILE), jnp.float32).at[block, obs_tile].add(score)
    spread = spread.reshape(N_SLAB, LEV, rows, NX // TILE, TILE)
    adjoint_field = jnp.transpose(spread, (1, 0, 2, 3, 4)).reshape(LEV, NY, NX)

    def adjoint(member_pert):
        weighted = rounded(member_pert.astype(jnp.float32) * adjoint_field)
        back = rounded(jnp.einsum('ay,lyx->lax', table_y, weighted))
        return amplitude * jnp.einsum('lax,xb->lab', back, table_x)
    return lax.map(adjoint, perturbation)
```

```python
import functools

import jax
import jax.numpy as jnp
from jax import lax
from jax.experimental import pallas as pl
from jax.experimental.pallas import tpu as pltpu
from jax.sharding import Mesh
from jax.sharding import PartitionSpec as P

TILE = 128
BF16 = jnp.bfloat16
F32 = jnp.float32
SLAB = ("chip", "core")
SAME_CORE = ("member", "chip")


def cost(flops, nbytes):
    return pl.CostEstimate(flops=flops, bytes_accessed=nbytes, transcendentals=0)


def whole(shape):
    return pl.BlockSpec(shape, lambda *_: (0,) * len(shape))


def angle(product, order):
    return (2.0 * jnp.pi / order) * (product % order).astype(F32)


def table_kernel(cos_ref, sin_ref, plus_ref, minus_ref, out_ref):
    plus = plus_ref[...]
    minus = minus_ref[...]
    rows = plus.shape[0]
    for p in range(16):
        c = jnp.broadcast_to(cos_ref[p][None], (rows // 16, 16, TILE)).reshape(rows, TILE)
        s = jnp.broadcast_to(sin_ref[p][None], (rows // 16, 16, TILE)).reshape(rows, TILE)
        out_ref[:, p * TILE : (p + 1) * TILE] = (c * plus + s * minus).astype(BF16)


def hartley_x(order):
    index = jnp.arange(order, dtype=jnp.int32)
    coarse = jnp.arange(16, dtype=jnp.int32)
    first = angle(coarse[:, None] * coarse[None, :], 16)
    cos_t = jnp.broadcast_to(jnp.cos(first)[:, :, None], (16, 16, TILE))
    sin_t = jnp.broadcast_to(jnp.sin(first)[:, :, None], (16, 16, TILE))
    second = angle(index[:, None] * index[None, :TILE], order)
    scale = 1.0 / jnp.sqrt(F32(order))
    plus = (jnp.cos(second) + jnp.sin(second)) * scale
    minus = (jnp.cos(second) - jnp.sin(second)) * scale
    step = 256
    return pl.pallas_call(
        table_kernel,
        grid=(order // step,),
        in_specs=[
            whole((16, 16, TILE)),
            whole((16, 16, TILE)),
            pl.BlockSpec((step, TILE), lambda i: (i, 0)),
            pl.BlockSpec((step, TILE), lambda i: (i, 0)),
        ],
        out_specs=pl.BlockSpec((step, order), lambda i: (i, 0)),
        out_shape=jax.ShapeDtypeStruct((order, order), BF16),
        cost_estimate=cost(order * order * 4, order * order * 2),
        name="table",
    )(cos_t, sin_t, plus, minus)


def hartley_rows(index, order):
    second = angle(index[:, None] * jnp.arange(order, dtype=jnp.int32)[None, :], order)
    return ((jnp.cos(second) + jnp.sin(second)) / jnp.sqrt(F32(order))).astype(BF16)


def select_kernel(index_ref, extra_ref, pert_ref, out_ref):
    members = pert_ref.shape[0]
    copies = out_ref.shape[0] // 2
    lane = lax.broadcasted_iota(jnp.int32, (16, TILE), 1)
    for k in range(16):
        chosen = (index_ref[16 * k : 16 * k + 16, :] == lane).astype(BF16)
        cols = slice(k * TILE, (k + 1) * TILE)
        tile = jnp.concatenate(
            [pert_ref[m, :, :, cols].reshape(TILE, TILE) for m in range(members)], axis=1
        )
        rows = jnp.dot(chosen, tile, preferred_element_type=F32).astype(BF16)
        for m in range(members):
            part = rows[:, m * TILE : (m + 1) * TILE]
            for h in range(copies):
                out_ref[2 * h + k // 8, (k % 8) * members + m] = part
    for h in range(copies):
        for c in range(2):
            out_ref[2 * h + c, 8 * members] = extra_ref[c]


def forward_kernel(core_ref, control_ref, row_ref, col_ref, table_ref, send_ref, own_ref, scaled):
    step = pl.program_id(0)
    members, levels, rows, width = control_ref.shape
    half = pl.num_programs(0) // 2

    @pl.when(step == 0)
    def _():
        for l in range(levels):
            amplitude = row_ref[l][:, :1] * col_ref[l : l + 1, :]
            for m in range(members):
                at = (m * levels + l) * rows
                scaled[at : at + rows, :] = (control_ref[m, l] * amplitude).astype(BF16)

    product = jnp.dot(scaled[...], table_ref[...], preferred_element_type=F32)
    product = product.astype(BF16).reshape(members, levels * rows, -1)

    @pl.when(step < half)
    def _():
        send_ref[...] = product

    @pl.when(step >= half)
    def _():
        own_ref[...] = product


def cells_kernel(pert_ref, extra_ref, own_ref, par_ref, rows_ref, cells_ref, spread_ref):
    kk = pl.program_id(0)
    members, depth, _ = own_ref.shape
    rows = depth // 2
    extra = extra_ref[:, 0, :8, :].astype(F32)
    mine = lax.broadcasted_iota(jnp.int32, (8, TILE), 0) == kk
    low = jnp.sum(jnp.where(mine, jnp.sum(extra[:8], axis=0), 0.0), axis=0, keepdims=True)
    high = jnp.sum(jnp.where(mine, jnp.sum(extra[8:], axis=0), 0.0), axis=0, keepdims=True)
    index = jnp.concatenate([low, high], axis=1).astype(jnp.int32)
    tiles = index.shape[1]
    source = lax.broadcasted_iota(jnp.int32, (1, tiles), 1) // 16
    y = source * rows + (index & (rows - 1))
    upper = index >= rows
    height = rows_ref.shape[1]
    chosen = (lax.broadcasted_iota(jnp.int32, (height, tiles), 0) == y).astype(F32).astype(BF16)
    picked = jnp.dot(rows_ref[...], chosen, preferred_element_type=F32)
    spread = jnp.concatenate(
        [jnp.where(upper, 0.0, picked), jnp.where(upper, picked, 0.0)], axis=0
    ).astype(BF16)
    spread_ref[0] = spread
    along = jnp.concatenate(
        [
            jnp.concatenate([ref[m, l * rows : (l + 1) * rows, :] for m in range(members)], axis=1)
            for l in range(2)
            for ref in (own_ref, par_ref)
        ],
        axis=0,
    )
    field = lax.dot_general(
        spread, along, (((0,), (0,)), ((), ())), preferred_element_type=F32
    )
    total = jnp.zeros((tiles, TILE), F32)
    for m in range(members):
        pert = pert_ref[:, m].reshape(tiles, TILE).astype(F32)
        total = total + pert * field[:, m * TILE : (m + 1) * TILE]
    cells_ref[0] = total.astype(BF16)


def score_kernel(cells_ref, value_ref, seen_ref, out_ref):
    copies = out_ref.shape[0]
    cells = jnp.sum(cells_ref[...].astype(F32), axis=0)
    resid = cells - value_ref[...]
    score = jnp.where(seen_ref[...] > 0.5, resid / jnp.sqrt(1.0 + resid * resid * 0.25), 0.0)
    score = score.astype(BF16)
    for i in range(copies):
        out_ref[i] = score


def back_kernel(pert_ref, score_ref, spread_ref, own_ref, par_ref):
    members, depth, _ = own_ref.shape
    rows = depth // 2
    score = score_ref[0].astype(F32)
    tiles = score.shape[0]
    weighted = jnp.concatenate(
        [
            (pert_ref[:, m].reshape(tiles, TILE).astype(F32) * score).astype(BF16)
            for m in range(members)
        ],
        axis=1,
    )
    back = jnp.dot(spread_ref[0], weighted, preferred_element_type=F32).astype(BF16)
    for l in range(2):
        for i, ref in enumerate((own_ref, par_ref)):
            at = (2 * l + i) * rows
            for m in range(members):
                ref[m, l * rows : (l + 1) * rows, :] = back[
                    at : at + rows, m * TILE : (m + 1) * TILE
                ]


def inverse_kernel(core_ref, own_ref, par_ref, row_ref, col_ref, mine_ref, other_ref, out_ref):
    members, levels, rows, width = out_ref.shape
    depth = own_ref.shape[2]
    own = own_ref[...].reshape(-1, depth)
    par = par_ref[...].reshape(-1, depth)
    product = jnp.dot(own, mine_ref[...], preferred_element_type=F32)
    product = product + jnp.dot(par, other_ref[...], preferred_element_type=F32)
    product = product.reshape(members, levels, rows, width)
    for l in range(levels):
        amplitude = row_ref[l][:, :1] * col_ref[l : l + 1, :]
        for m in range(members):
            out_ref[m, l] = product[m, l] * amplitude


def shards(control, perturbation, loc_row, loc_col, obs_tile, obs_count, obs_value):
    members, levels, rows, width = control.shape
    chips = lax.axis_size("chip")
    slabs = chips * 2
    peers = lax.axis_size("member") * chips
    height = rows * slabs
    half = width // 2
    per_core = half // TILE
    chip = lax.axis_index("chip")
    core = lax.axis_index("core")
    slab = chip * 2 + core
    group = lax.axis_index("member")
    swap = [(0, 1), (1, 0)]

    place = obs_tile // (width // TILE)
    index = jnp.broadcast_to(place[:, None], (slabs * 16, TILE))
    lane = jnp.arange(TILE, dtype=jnp.int32)
    extra = jnp.where(
        lane[None, :] // 16 == slab % 8, jnp.tile(place.reshape(slabs, 16), (1, 8)), 0
    ).astype(BF16)
    extra = jnp.pad(extra.reshape(2, 8, TILE), ((0, 0), (0, 8), (0, 0)))
    blocks = per_core * members
    message = pl.pallas_call(
        select_kernel,
        out_shape=jax.ShapeDtypeStruct((slabs, blocks + 1, 16, TILE), BF16),
        cost_estimate=cost(2 * 256 * TILE * TILE * members, 5 << 20),
        name="select",
    )(index, extra, perturbation)
    arrived = lax.all_to_all(message, SLAB, split_axis=0, concat_axis=0, tiled=True)

    def of_column(column, array):
        return lax.dynamic_slice_in_dim(array, column * 16, 16, 0)

    seen = (lane[None, :] < obs_count[:, None]).astype(F32)
    mine = per_core * core + group
    other = per_core * (1 - core) + group
    stated = jnp.stack([of_column(mine, obs_value), of_column(mine, seen)])
    lent = jnp.stack([of_column(other, obs_value), of_column(other, seen)])
    lent = lax.ppermute(lent, "core", swap)
    stated = jnp.where(
        core == 0,
        jnp.concatenate([stated, lent], axis=1),
        jnp.concatenate([lent, stated], axis=1),
    )

    table = hartley_x(width)
    row_b = jnp.broadcast_to(loc_row[:, :, None], (levels, rows, TILE))
    core_index = core.astype(jnp.int32).reshape(1)
    wide = 256
    steps = width // wide
    send, own = pl.pallas_call(
        forward_kernel,
        grid_spec=pltpu.PrefetchScalarGridSpec(
            num_scalar_prefetch=1,
            grid=(steps,),
            in_specs=[
                whole(control.shape),
                whole(row_b.shape),
                whole(loc_col.shape),
                pl.BlockSpec(
                    (width, wide), lambda i, c: (0, lax.rem(i + (steps // 2) * (1 - c[0]), steps))
                ),
            ],
            out_specs=[
                pl.BlockSpec(
                    (members, levels * rows, wide),
                    lambda i, c: (0, 0, jnp.minimum(i, steps // 2 - 1)),
                ),
                pl.BlockSpec(
                    (members, levels * rows, wide),
                    lambda i, c: (0, 0, jnp.maximum(i - steps // 2, 0)),
                ),
            ],
            scratch_shapes=[pltpu.VMEM((members * levels * rows, width), BF16)],
        ),
        out_shape=[jax.ShapeDtypeStruct((members, levels * rows, half), BF16)] * 2,
        cost_estimate=cost(2 * members * levels * rows * width * width, 14 << 20),
        name="forward",
    )(core_index, control, row_b, loc_col, table)
    par = lax.ppermute(send, "core", swap)

    near = jnp.arange(rows, dtype=jnp.int32)
    near = jnp.concatenate([slab * rows + near, (chip * 2 + 1 - core) * rows + near])
    table_rows = hartley_rows(near, height)
    tiles = slabs * 16
    pert_spec = pl.BlockSpec((slabs, members, 16, TILE), lambda k: (0, k, 0, 0))
    part_spec = pl.BlockSpec((members, levels * rows, TILE), lambda k: (0, 0, k))
    cells, spread = pl.pallas_call(
        cells_kernel,
        grid=(per_core,),
        in_specs=[
            pert_spec,
            pl.BlockSpec((slabs, 1, 16, TILE), lambda k: (0, blocks, 0, 0)),
            part_spec,
            part_spec,
            whole(table_rows.shape),
        ],
        out_specs=[
            pl.BlockSpec((1, tiles, TILE), lambda k: (k, 0, 0)),
            pl.BlockSpec((1, 4 * rows, tiles), lambda k: (k, 0, 0)),
        ],
        out_shape=[
            jax.ShapeDtypeStruct((per_core, tiles, TILE), BF16),
            jax.ShapeDtypeStruct((per_core, 4 * rows, tiles), BF16),
        ],
        cost_estimate=cost(1 << 30, 6 << 20),
        name="cells",
    )(arrived, arrived, own, par, table_rows)
    cells = lax.all_to_all(
        cells.reshape(peers, 2 * 16, TILE), SAME_CORE, split_axis=0, concat_axis=0, tiled=True
    )
    score = pl.pallas_call(
        score_kernel,
        out_shape=jax.ShapeDtypeStruct((peers, 2 * 16, TILE), BF16),
        name="score",
    )(cells, stated[0], stated[1])
    score = lax.all_to_all(score, SAME_CORE, split_axis=0, concat_axis=0, tiled=True)

    back_own, back_send = pl.pallas_call(
        back_kernel,
        grid=(per_core,),
        in_specs=[
            pert_spec,
            pl.BlockSpec((1, tiles, TILE), lambda k: (k, 0, 0)),
            pl.BlockSpec((1, 4 * rows, tiles), lambda k: (k, 0, 0)),
        ],
        out_specs=[part_spec, part_spec],
        out_shape=[jax.ShapeDtypeStruct((members, levels * rows, half), BF16)] * 2,
        cost_estimate=cost(1 << 29, 6 << 20),
        name="back",
    )(arrived, score.reshape(per_core, tiles, TILE), spread)
    back_par = lax.ppermute(back_send, "core", swap)

    return pl.pallas_call(
        inverse_kernel,
        grid_spec=pltpu.PrefetchScalarGridSpec(
            num_scalar_prefetch=1,
            grid=(steps,),
            in_specs=[
                whole(back_own.shape),
                whole(back_par.shape),
                whole(row_b.shape),
                pl.BlockSpec((levels, wide), lambda i, c: (0, i)),
                pl.BlockSpec((half, wide), lambda i, c: (c[0], i)),
                pl.BlockSpec((half, wide), lambda i, c: (1 - c[0], i)),
            ],
            out_specs=pl.BlockSpec((members, levels, rows, wide), lambda i, c: (0, 0, 0, i)),
        ),
        out_shape=jax.ShapeDtypeStruct(control.shape, F32),
        cost_estimate=cost(2 * members * levels * rows * width * width, 14 << 20),
        name="inverse",
    )(core_index, back_own, back_par, row_b, loc_col, table, table)


def solution(mesh):
    torus = Mesh(
        mesh.devices.reshape(mesh.shape["member"], mesh.shape["slab"] // 2, 2),
        ("member", "chip", "core"),
    )
    placed = (
        P("member", None, SLAB, None),
        P("member", None, SLAB, None),
        P(None, SLAB),
        P(),
        P(SLAB),
        P(SLAB),
        P(SLAB, None),
    )
    return jax.shard_map(
        shards,
        mesh=torus,
        in_specs=placed,
        out_specs=P("member", None, SLAB, None),
        check_vma=False,
    )
```

```python
import jax
import jax.numpy as jnp
import numpy as np
from jax import lax
from jax.experimental import pallas as pl
from jax.experimental.pallas import tpu as pltpu
from jax.sharding import Mesh
from jax.sharding import PartitionSpec as P

TILE = 128
WIDE = 256
BF16 = jnp.bfloat16
F32 = jnp.float32
SLAB = ("chip", "core")
SAME_CORE = ("member", "chip")
VMEM = pl.BlockSpec(memory_space=pltpu.VMEM)
SMEM = pl.BlockSpec(memory_space=pltpu.SMEM)
HBM = pl.BlockSpec(memory_space=pltpu.HBM)


def run(kernel, out_shape, in_specs, mib, flops, scratch=(), out_specs=None):
    outs = out_shape if isinstance(out_shape, list) else [out_shape]
    if out_specs is None:
        out_specs = [VMEM] * len(outs)
    moved = sum(int(np.prod(o.shape)) * o.dtype.itemsize for o in outs) * 2
    call = pl.pallas_call(
        kernel,
        in_specs=in_specs,
        out_specs=out_specs,
        out_shape=outs,
        scratch_shapes=list(scratch),
        compiler_params=pltpu.CompilerParams(vmem_limit_bytes=mib << 20),
        cost_estimate=pl.CostEstimate(flops=flops, bytes_accessed=moved, transcendentals=0),
        name=kernel.__name__,
    )
    if isinstance(out_shape, list):
        return call
    return lambda *args: call(*args)[0]


def bf16(*shape):
    return jax.ShapeDtypeStruct(shape, BF16)


def f32(*shape):
    return jax.ShapeDtypeStruct(shape, F32)


def cas(first, second, order):
    angle = 2.0 * np.pi * (np.outer(first, second) % order) / order
    c, s = np.cos(angle), np.sin(angle)
    return [a.astype(np.float32) for a in (c + s, c - s, c, s)]


def select(core_ref, tile_ref, pert_ref, own_ref, send_ref):
    members = pert_ref.shape[0]
    core = core_ref[0]
    place = tile_ref[...] // 16
    row = lax.broadcasted_iota(jnp.int32, (TILE, TILE), 0)
    for ref, half in ((send_ref, 1 - core), (own_ref, core)):
        mine = jnp.where(half == 0, place[0:1, :], place[1:2, :])
        chosen = jnp.transpose((row == mine).astype(F32)).astype(BF16)
        for k in range(8):
            cols = pl.ds(pl.multiple_of((half * 8 + k) * TILE, TILE), TILE)
            tile = jnp.concatenate(
                [pert_ref[m, :, :, cols].reshape(TILE, TILE) for m in range(members)], axis=1
            )
            rows = jnp.dot(
                chosen[16 * k : 16 * k + 16], tile, preferred_element_type=F32
            ).astype(BF16)
            for m in range(members):
                ref[k * members + m] = rows[:, m * TILE : (m + 1) * TILE]
        ref[8 * members] = jnp.broadcast_to(mine.astype(F32), (16, TILE)).astype(BF16)


def forward(
    core_ref, control_ref, row_ref, col_ref,
    outer_c, outer_s, inner_p, inner_m, lead_c, lead_s,
    send_ref, own_ref, table_ref, scaled, plus, minus, block_ref, sems,
):
    members, levels, rows, width = control_ref.shape
    core = core_ref[0]
    steps = width // WIDE
    half = steps // 2
    block = inner_p.shape[0]
    for u in range(width // block):
        at = slice(u * block, (u + 1) * block)
        c, s = outer_c[u : u + 1, :], outer_s[u : u + 1, :]
        plus[at, :] = c * inner_p[...] + s * inner_m[...]
        minus[at, :] = c * inner_m[...] - s * inner_p[...]
    for l in range(levels):
        amplitude = row_ref[l][:, :1] * col_ref[l : l + 1, :]
        for m in range(members):
            at = (m * levels + l) * rows
            scaled[at : at + rows, :] = (control_ref[m, l] * amplitude).astype(BF16)

    def copy(nb, slot):
        return pltpu.make_async_copy(block_ref.at[slot], table_ref.at[nb], sems.at[slot])

    def step(which, target, n):
        nb = which * half + n
        slot = lax.rem(n, 2)

        @pl.when(n >= 2)
        def _():
            copy(nb, slot).wait()

        for q in range(WIDE // TILE):
            c = lead_c[nb * (WIDE // TILE) + q]
            s = lead_s[nb * (WIDE // TILE) + q]
            c = jnp.broadcast_to(c[None], (width // 16, 16, TILE)).reshape(width, TILE)
            s = jnp.broadcast_to(s[None], (width // 16, 16, TILE)).reshape(width, TILE)
            block_ref[slot, :, q * TILE : (q + 1) * TILE] = (
                c * plus[...] + s * minus[...]
            ).astype(BF16)
        copy(nb, slot).start()
        product = jnp.dot(scaled[...], block_ref[slot], preferred_element_type=F32)
        to = pl.ds(pl.multiple_of(n * WIDE, WIDE), WIDE)
        target[:, :, to] = product.astype(BF16).reshape(members, levels * rows, WIDE)

    def drain():
        for slot in range(2):
            copy(0, slot).wait()

    lax.fori_loop(0, half, lambda n, _: (step(1 - core, send_ref, n), 0)[1], 0)
    drain()
    lax.fori_loop(0, half, lambda n, _: (step(core, own_ref, n), 0)[1], 0)
    drain()


def spread_rows(place_ref, inner_p, inner_m, lead_c, lead_s, lane_c, lane_s, out_ref):
    chip, core = place_ref[0], place_ref[1]
    rows = inner_p.shape[0]
    plus, minus = [], []
    for q in range(2):
        slab = chip * 2 + (core + q) % 2
        c = jnp.broadcast_to(lead_c[slab][None], (rows // 16, 16, TILE)).reshape(rows, TILE)
        s = jnp.broadcast_to(lead_s[slab][None], (rows // 16, 16, TILE)).reshape(rows, TILE)
        plus.append(c * inner_p[...] + s * inner_m[...])
        minus.append(c * inner_m[...] - s * inner_p[...])
    left = lax.broadcasted_iota(jnp.int32, (rows, TILE), 1) < rows
    plus = jnp.where(left, plus[0], plus[1])
    minus = jnp.where(left, minus[0], minus[1])
    nothing = jnp.zeros((rows, TILE), BF16)
    for h in range(out_ref.shape[0]):
        for r in range(2):
            slab = h * 2 + (core + r) % 2
            entry = (lane_c[pl.ds(slab, 1), :] * plus + lane_s[pl.ds(slab, 1), :] * minus).astype(BF16)
            for l in range(2):
                at = slice((2 * l + r) * rows, (2 * l + r + 1) * rows)
                out_ref[h, at, l * TILE : (l + 1) * TILE] = entry
                out_ref[h, at, (1 - l) * TILE : (2 - l) * TILE] = nothing


def tiles_of(ref, k):
    chips = ref.shape[0]
    return jnp.concatenate(
        [
            ref[h, r * TILE + k * 16 : r * TILE + (k + 1) * 16, :]
            for h in range(chips)
            for r in range(2)
        ],
        axis=0,
    )


def cells(pert_ref, own_ref, par_ref, rows_ref, cells_ref, spread_ref):
    members, depth, _ = own_ref.shape
    rows = depth // 2
    chips = pert_ref.shape[0]
    last = pert_ref.shape[2] - 1
    lane = lax.broadcasted_iota(jnp.int32, (1, 2 * TILE), 1)
    row = lax.broadcasted_iota(jnp.int32, (4 * rows, 2 * TILE), 0)
    for h in range(chips):
        place = jnp.concatenate(
            [pert_ref[h, r, last].astype(F32)[0:1, :] for r in range(2)], axis=1
        ).astype(jnp.int32)
        level, inside = place // rows, place % rows
        place = level * (2 * rows) + inside + jnp.where(lane < TILE, 0, rows)
        chosen = (row == place).astype(F32).astype(BF16)
        spread_ref[h] = lax.dot_general(
            chosen, rows_ref[h], (((0,), (0,)), ((), ())), preferred_element_type=F32
        ).astype(BF16)
    for k in range(8):
        cols = slice(k * TILE, (k + 1) * TILE)
        along = jnp.concatenate(
            [
                jnp.concatenate(
                    [ref[m, l * rows : (l + 1) * rows, cols] for m in range(members)], axis=1
                )
                for l in range(2)
                for ref in (own_ref, par_ref)
            ],
            axis=0,
        )
        field = jnp.dot(tiles_of(spread_ref, k), along, preferred_element_type=F32)
        total = None
        for m in range(members):
            pert = pert_ref[:, :, k * members + m].reshape(-1, TILE).astype(F32)
            term = pert * field[:, m * TILE : (m + 1) * TILE]
            total = term if total is None else total + term
        cells_ref[k] = total.astype(BF16)


def turn(spread_ref, own_ref, par_ref):
    rows = own_ref.shape[1] // 2
    for k in range(8):
        turned = jnp.transpose(tiles_of(spread_ref, k).astype(F32)).astype(BF16)
        for l in range(2):
            to = slice(l * rows, (l + 1) * rows)
            own_ref[k, to, :] = turned[2 * l * rows : (2 * l + 1) * rows]
            par_ref[k, to, :] = turned[(2 * l + 1) * rows : (2 * l + 2) * rows]


def score(cells_ref, own_ref, lent_ref, out_ref):
    copies = out_ref.shape[0]
    total = jnp.sum(cells_ref[...].astype(F32), axis=0)
    value = jnp.concatenate([own_ref[0], lent_ref[0]], axis=0)
    seen = jnp.concatenate([own_ref[1], lent_ref[1]], axis=0)
    resid = total - value
    result = jnp.where(seen > 0.5, resid / jnp.sqrt(1.0 + resid * resid * 0.25), 0.0)
    result = result.astype(BF16)
    for i in range(copies):
        out_ref[i] = result


def to_members(ref, k, back):
    for m in range(ref.shape[0]):
        ref[m, :, k * TILE : (k + 1) * TILE] = back[:, m * TILE : (m + 1) * TILE]


def back_par(pert_ref, score_ref, turned_ref, weighted_ref, par_ref):
    members = par_ref.shape[0]
    for k in range(8):
        weight = score_ref[k].astype(F32)
        weighted = jnp.concatenate(
            [
                (pert_ref[:, :, k * members + m].reshape(-1, TILE).astype(F32) * weight).astype(BF16)
                for m in range(members)
            ],
            axis=1,
        )
        weighted_ref[k] = weighted
        to_members(
            par_ref, k, jnp.dot(turned_ref[k], weighted, preferred_element_type=F32).astype(BF16)
        )


def inverse_own(core_ref, weighted_ref, turned_ref, table_ref, sum_ref, own, block_ref, sems):
    members, depth, width = own.shape
    steps = sum_ref.shape[0]
    near = pl.ds(pl.multiple_of(core_ref[0] * width, width), width)

    def fetch(n, slot):
        return pltpu.make_async_copy(
            table_ref.at[n, near, :], block_ref.at[slot], sems.at[slot]
        )

    fetch(0, 0).start()
    for k in range(8):
        to_members(
            own,
            k,
            jnp.dot(turned_ref[k], weighted_ref[k], preferred_element_type=F32).astype(BF16),
        )

    def step(n, carry):
        slot = lax.rem(n, 2)

        @pl.when(n + 1 < steps)
        def _():
            fetch(n + 1, 1 - slot).start()

        fetch(n, slot).wait()
        sum_ref[n] = jnp.dot(
            own[...].reshape(members * depth, width),
            block_ref[slot],
            preferred_element_type=F32,
        )
        return carry

    lax.fori_loop(0, steps, step, 0)


def inverse_par(
    core_ref, par_ref, sum_ref, table_ref, row_ref, col_ref, out_ref, piece, sems, block_ref, reads
):
    members, depth, width = par_ref.shape
    levels, rows, _ = row_ref.shape
    steps = sum_ref.shape[0]
    far = pl.ds(pl.multiple_of((1 - core_ref[0]) * width, width), width)

    def fetch(n, slot):
        return pltpu.make_async_copy(
            table_ref.at[n, far, :], block_ref.at[slot], reads.at[slot]
        )

    fetch(0, 0).start()

    def copy(n, slot):
        cols = pl.ds(pl.multiple_of(n * WIDE, WIDE), WIDE)
        return pltpu.make_async_copy(piece.at[slot], out_ref.at[:, :, :, cols], sems.at[slot])

    def step(n, carry):
        slot = lax.rem(n, 2)
        cols = pl.ds(pl.multiple_of(n * WIDE, WIDE), WIDE)

        @pl.when(n + 1 < steps)
        def _():
            fetch(n + 1, 1 - slot).start()

        fetch(n, slot).wait()
        product = sum_ref[n] + jnp.dot(
            par_ref[...].reshape(members * depth, width),
            block_ref[slot],
            preferred_element_type=F32,
        )
        product = product.reshape(members, levels, rows, WIDE)

        @pl.when(n >= 2)
        def _():
            copy(n - 2, slot).wait()

        for l in range(levels):
            amplitude = row_ref[l][:, :1] * col_ref[l : l + 1, cols]
            for m in range(members):
                piece[slot, m, l] = product[m, l] * amplitude
        copy(n, slot).start()
        return carry

    lax.fori_loop(0, steps, step, 0)
    copy(steps - 2, steps % 2).wait()
    copy(steps - 1, (steps - 1) % 2).wait()


def shards(control, perturbation, loc_row, loc_col, obs_tile, obs_count, obs_value):
    members, levels, rows, width = control.shape
    chips = lax.axis_size("chip")
    slabs = chips * 2
    peers = lax.axis_size("member") * chips
    height = rows * slabs
    half = width // 2
    per_core = half // TILE
    depth = levels * rows
    chip = lax.axis_index("chip").astype(jnp.int32)
    core = lax.axis_index("core").astype(jnp.int32)
    group = lax.axis_index("member").astype(jnp.int32)
    core_index = core.reshape(1)
    swap = [(0, 1), (1, 0)]

    blocks = per_core * members + 1
    own_tiles, send_tiles = run(
        select, [bf16(blocks, 16, TILE)] * 2, [SMEM, VMEM, VMEM], 16, 1 << 27
    )(core_index, obs_tile.reshape(2, TILE), perturbation)
    par_tiles = lax.ppermute(send_tiles, "core", swap)
    message = jnp.broadcast_to(
        jnp.stack([own_tiles, par_tiles])[None], (chips, 2, blocks, 16, TILE)
    )
    arrived = lax.all_to_all(message, "chip", split_axis=0, concat_axis=0, tiled=True)

    lane = jnp.arange(TILE, dtype=jnp.int32)

    def of_column(column, array):
        return lax.dynamic_slice_in_dim(array, column * 16, 16, 0)

    seen = (lane[None, :] < obs_count[:, None]).astype(F32)
    mine = per_core * core + group
    other = per_core * (1 - core) + group
    stated = jnp.stack([of_column(mine, obs_value), of_column(mine, seen)])
    lent = jnp.stack([of_column(other, obs_value), of_column(other, seen)])
    lent = lax.ppermute(lent, "core", swap)

    lead = cas(np.arange(16), np.arange(16), 16)
    lead_c, lead_s = [jnp.asarray(np.repeat(a[:, :, None], TILE, axis=2)) for a in lead[2:]]
    inner = 64
    outer = cas(np.arange(width // inner), np.arange(TILE), width // inner)
    outer_c, outer_s = [jnp.asarray(a) for a in outer[2:]]
    near = cas(np.arange(inner), np.arange(TILE), width)
    near_p, near_m = [jnp.asarray(a / np.float32(np.sqrt(width))) for a in near[:2]]
    wave = np.arange(TILE) % rows
    base = cas(np.arange(rows), wave, height)
    base_p, base_m = [jnp.asarray(a / np.float32(np.sqrt(height))) for a in base[:2]]
    lane_c, lane_s = [jnp.asarray(a) for a in cas(np.arange(16), wave, 16)[2:]]

    row_b = jnp.broadcast_to(loc_row[:, :, None], (levels, rows, TILE))
    send, own, table = run(
        forward,
        [bf16(members, depth, half), bf16(members, depth, half), bf16(width // WIDE, width, WIDE)],
        [SMEM] + [VMEM] * 9,
        24,
        2 * members * depth * width * width,
        [
            pltpu.VMEM((members * depth, width), BF16),
            pltpu.VMEM((width, TILE), F32),
            pltpu.VMEM((width, TILE), F32),
            pltpu.VMEM((2, width, WIDE), BF16),
            pltpu.SemaphoreType.DMA((2,)),
        ],
        [VMEM, VMEM, HBM],
    )(core_index, control, row_b, loc_col, outer_c, outer_s, near_p, near_m, lead_c, lead_s)
    par = lax.ppermute(send, "core", swap)
    table_rows = run(
        spread_rows, bf16(chips, 4 * rows, 2 * TILE), [SMEM] + [VMEM] * 6, 4, 1 << 22
    )(jnp.stack([chip, core]), base_p, base_m, lead_c, lead_s, lane_c, lane_s)

    tiles = slabs * 16
    partial, spread = run(
        cells,
        [bf16(per_core, tiles, TILE), bf16(chips, tiles, 4 * rows)],
        [VMEM] * 4,
        12,
        1 << 30,
    )(arrived, own, par, table_rows)
    partial = lax.all_to_all(
        partial.reshape(peers, 2 * 16, TILE), SAME_CORE, split_axis=0, concat_axis=0, tiled=True
    )
    turned, turned_par = run(
        turn, [bf16(per_core, depth, tiles), bf16(per_core, depth, tiles)], [VMEM], 6, 1 << 22
    )(spread)
    scores = run(score, bf16(peers, 2 * 16, TILE), [VMEM] * 3, 4, 1 << 20)(partial, stated, lent)
    scores = lax.all_to_all(scores, SAME_CORE, split_axis=0, concat_axis=0, tiled=True)

    weighted, back_send = run(
        back_par,
        [bf16(per_core, tiles, members * TILE), bf16(members, depth, half)],
        [VMEM] * 3,
        12,
        1 << 28,
    )(arrived, scores.reshape(per_core, tiles, TILE), turned_par)
    back_other = lax.ppermute(back_send, "core", swap)
    summed = run(
        inverse_own,
        f32(width // WIDE, members * depth, WIDE),
        [SMEM, VMEM, VMEM, HBM],
        14,
        members * depth * width * width,
        [
            pltpu.VMEM((members, depth, half), BF16),
            pltpu.VMEM((2, half, WIDE), BF16),
            pltpu.SemaphoreType.DMA((2,)),
        ],
    )(core_index, weighted, turned, table)
    return run(
        inverse_par,
        f32(*control.shape),
        [SMEM, VMEM, VMEM, HBM, VMEM, VMEM],
        14,
        members * depth * width * width,
        [
            pltpu.VMEM((2, members, levels, rows, WIDE), F32),
            pltpu.SemaphoreType.DMA((2,)),
            pltpu.VMEM((2, half, WIDE), BF16),
            pltpu.SemaphoreType.DMA((2,)),
        ],
        [HBM],
    )(core_index, back_other, summed, table, row_b, loc_col)


def solution(mesh):
    torus = Mesh(
        mesh.devices.reshape(mesh.shape["member"], mesh.shape["slab"] // 2, 2),
        ("member", "chip", "core"),
    )
    placed = (
        P("member", None, SLAB, None),
        P("member", None, SLAB, None),
        P(None, SLAB),
        P(),
        P(SLAB),
        P(SLAB),
        P(SLAB, None),
    )
    return jax.shard_map(
        shards,
        mesh=torus,
        in_specs=placed,
        out_specs=P("member", None, SLAB, None),
        check_vma=False,
    )
```

```python
import jax
import jax.numpy as jnp
import numpy as np
from jax import lax
from jax.experimental import pallas as pl
from jax.experimental.pallas import tpu as pltpu
from jax.sharding import Mesh
from jax.sharding import PartitionSpec as P

TILE = 128
WIDE = 256
BF16 = jnp.bfloat16
F32 = jnp.float32
SLAB = ("across", "along", "core")
SAME_CORE = ("member", "across", "along")
VMEM = pl.BlockSpec(memory_space=pltpu.VMEM)
SMEM = pl.BlockSpec(memory_space=pltpu.SMEM)
HBM = pl.BlockSpec(memory_space=pltpu.HBM)


def run(kernel, out_shape, in_specs, flops, scratch=(), out_specs=None, mib=60):
    outs = out_shape if isinstance(out_shape, list) else [out_shape]
    if out_specs is None:
        out_specs = [VMEM] * len(outs)
    moved = sum(int(np.prod(o.shape)) * o.dtype.itemsize for o in outs) * 2
    call = pl.pallas_call(
        kernel,
        in_specs=in_specs,
        out_specs=out_specs,
        out_shape=outs,
        scratch_shapes=list(scratch),
        compiler_params=pltpu.CompilerParams(vmem_limit_bytes=mib << 20),
        cost_estimate=pl.CostEstimate(flops=flops, bytes_accessed=moved, transcendentals=0),
    )

    def launch(*args):
        results = call(*args)
        return results if isinstance(out_shape, list) else results[0]

    return launch


def bf16(*shape):
    return jax.ShapeDtypeStruct(shape, BF16)


def f32(*shape):
    return jax.ShapeDtypeStruct(shape, F32)


def cas(first, second, order):
    angle = 2.0 * np.pi * (np.outer(first, second) % order) / order
    c, s = np.cos(angle), np.sin(angle)
    return [a.astype(np.float32) for a in (c + s, c - s, c, s)]


def select(core_ref, tile_ref, pert_ref, own_ref, send_ref, tiles, pert, sems):
    members = pert.shape[0]
    core = core_ref[0]
    copies = [pltpu.make_async_copy(tile_ref, tiles, sems.at[members])]
    copies += [pltpu.make_async_copy(pert_ref.at[m], pert.at[m], sems.at[m]) for m in range(members)]
    for copy in copies:
        copy.start()
    copies[0].wait()
    place = tiles[...] // 16
    row = lax.broadcasted_iota(jnp.int32, (TILE, TILE), 0)
    halves = []
    for half in (1 - core, core):
        mine = jnp.where(half == 0, place[0:1, :], place[1:2, :])
        halves.append((mine, jnp.transpose((row == mine).astype(F32)).astype(BF16)))
    for copy in copies[1:]:
        copy.wait()
    for ref, half, (mine, chosen) in zip((send_ref, own_ref), (1 - core, core), halves):
        for k in range(8):
            cols = pl.ds(pl.multiple_of((half * 8 + k) * TILE, TILE), TILE)
            tile = jnp.concatenate(
                [pert[m, :, :, cols].reshape(TILE, TILE) for m in range(members)], axis=1
            )
            rows = jnp.dot(
                chosen[16 * k : 16 * k + 16], tile, preferred_element_type=F32
            ).astype(BF16)
            for m in range(members):
                ref[k * members + m] = rows[:, m * TILE : (m + 1) * TILE]
        ref[8 * members] = jnp.broadcast_to(mine.astype(F32), (16, TILE)).astype(BF16)


def table_factors(factor_ref, width, plus, minus):
    inner = 64
    outer = width // inner
    near_p = factor_ref[2 * outer : 2 * outer + inner, :]
    near_m = factor_ref[2 * outer + inner : 2 * outer + 2 * inner, :]
    for u in range(outer):
        at = slice(u * inner, (u + 1) * inner)
        c, s = factor_ref[u : u + 1, :], factor_ref[outer + u : outer + u + 1, :]
        plus[at, :] = c * near_p + s * near_m
        minus[at, :] = c * near_m - s * near_p


def transform(which, scaled, lead_ref, plus, minus, block_ref, table_ref, sems, target):
    width = plus.shape[0]
    members, depth, _ = target.shape
    half = width // WIDE // 2

    def copy(nb, slot):
        return pltpu.make_async_copy(block_ref.at[slot], table_ref.at[nb], sems.at[slot])

    def step(n, carry):
        nb = which * half + n
        slot = lax.rem(n, 2)

        @pl.when(n >= 2)
        def _():
            copy(n - 2, slot).wait()

        for q in range(WIDE // TILE):
            c = lead_ref[0, nb * (WIDE // TILE) + q]
            s = lead_ref[1, nb * (WIDE // TILE) + q]
            c = jnp.broadcast_to(c[None], (width // 16, 16, TILE)).reshape(width, TILE)
            s = jnp.broadcast_to(s[None], (width // 16, 16, TILE)).reshape(width, TILE)
            block_ref[slot, :, q * TILE : (q + 1) * TILE] = (
                c * plus[...] + s * minus[...]
            ).astype(BF16)
        copy(n, slot).start()
        product = jnp.dot(scaled[...], block_ref[slot], preferred_element_type=F32)
        to = pl.ds(pl.multiple_of(n * WIDE, WIDE), WIDE)
        target[:, :, to] = product.astype(BF16).reshape(members, depth, WIDE)
        return carry

    lax.fori_loop(0, half, step, 0)
    for slot in range(2):
        copy(slot, slot).wait()


def forward_send(
    core_ref, control_ref, row_ref, col_ref, factor_ref, lead_ref, after_ref,
    send_ref, scaled_ref, table_ref,
    control, plus, minus, block_ref, sems, reads,
):
    members, levels, rows, width = control.shape
    copies = [
        pltpu.make_async_copy(control_ref.at[m], control.at[m], reads.at[m]) for m in range(members)
    ]
    for copy in copies:
        copy.start()
    table_factors(factor_ref, width, plus, minus)
    for m in range(members):
        copies[m].wait()
        for l in range(levels):
            amplitude = row_ref[l][:, :1] * col_ref[l : l + 1, :]
            at = (m * levels + l) * rows
            scaled_ref[at : at + rows, :] = (control[m, l] * amplitude).astype(BF16)
    transform(
        1 - core_ref[0], scaled_ref, lead_ref, plus, minus, block_ref, table_ref, sems, send_ref
    )


def forward_own(
    core_ref, scaled_ref, factor_ref, lead_ref, after0_ref, after1_ref,
    own_ref, table_ref, plus, minus, block_ref, sems,
):
    table_factors(factor_ref, plus.shape[0], plus, minus)
    transform(core_ref[0], scaled_ref, lead_ref, plus, minus, block_ref, table_ref, sems, own_ref)


def chip_of(place_ref, h):
    across, along = place_ref[0], place_ref[1]
    return ((across + h // 4) % 2) * 4 + (along + h % 4) % 4


def spread_rows(place_ref, factor_ref, lead_ref, out_ref):
    core = place_ref[2]
    rows = out_ref.shape[1] // 4
    inner_p, inner_m = factor_ref[:rows, :], factor_ref[rows : 2 * rows, :]
    plus, minus = [], []
    for q in range(2):
        slab = chip_of(place_ref, 0) * 2 + (core + q) % 2
        c = jnp.broadcast_to(lead_ref[0, slab][None], (rows // 16, 16, TILE)).reshape(rows, TILE)
        s = jnp.broadcast_to(lead_ref[1, slab][None], (rows // 16, 16, TILE)).reshape(rows, TILE)
        plus.append(c * inner_p + s * inner_m)
        minus.append(c * inner_m - s * inner_p)
    left = lax.broadcasted_iota(jnp.int32, (rows, TILE), 1) < rows
    plus = jnp.where(left, plus[0], plus[1])
    minus = jnp.where(left, minus[0], minus[1])
    nothing = jnp.zeros((rows, TILE), BF16)
    for h in range(out_ref.shape[0]):
        for r in range(2):
            slab = chip_of(place_ref, h) * 2 + (core + r) % 2
            c = factor_ref[pl.ds(2 * rows + slab, 1), :]
            s = factor_ref[pl.ds(2 * rows + 16 + slab, 1), :]
            entry = (c * plus + s * minus).astype(BF16)
            for l in range(2):
                at = slice((2 * l + r) * rows, (2 * l + r + 1) * rows)
                out_ref[h, at, l * TILE : (l + 1) * TILE] = entry
                out_ref[h, at, (1 - l) * TILE : (2 - l) * TILE] = nothing


def pert_of(blocks, at):
    return jnp.concatenate([ref[:, at].reshape(-1, TILE) for ref in blocks], axis=0).astype(F32)


def cells(place_ref, *refs):
    blocks, (own_hbm, par_hbm, rows_ref, cells_hbm, turned_hbm) = refs[:8], refs[8:13]
    own, par, spread, cells_ref, turned_ref, reads, writes = refs[13:]
    members, depth, _ = own.shape
    rows = depth // 2
    last = blocks[0].shape[1] - 1
    loads = [
        pltpu.make_async_copy(own_hbm, own, reads.at[0]),
        pltpu.make_async_copy(par_hbm, par, reads.at[1]),
    ]
    for load in loads:
        load.start()
    lane = lax.broadcasted_iota(jnp.int32, (1, 2 * TILE), 1)
    row = lax.broadcasted_iota(jnp.int32, (4 * rows, 2 * TILE), 0)
    for h, block in enumerate(blocks):
        place = jnp.concatenate(
            [block[r, last].astype(F32)[0:1, :] for r in range(2)], axis=1
        ).astype(jnp.int32)
        level, inside = place // rows, place % rows
        place = level * (2 * rows) + inside + jnp.where(lane < TILE, 0, rows)
        chosen = (row == place).astype(F32).astype(BF16)
        spread[h] = lax.dot_general(
            chosen, rows_ref[h], (((0,), (0,)), ((), ())), preferred_element_type=F32
        ).astype(BF16)
    for load in loads:
        load.wait()
    stores = []
    for k in range(8):
        cols = slice(k * TILE, (k + 1) * TILE)
        along = jnp.concatenate(
            [
                jnp.concatenate(
                    [ref[m, l * rows : (l + 1) * rows, cols] for m in range(members)], axis=1
                )
                for l in range(2)
                for ref in (own, par)
            ],
            axis=0,
        )
        tiles = jnp.concatenate(
            [
                spread[h, r * TILE + k * 16 : r * TILE + (k + 1) * 16, :]
                for h in range(8)
                for r in range(2)
            ],
            axis=0,
        )
        field = jnp.dot(tiles, along, preferred_element_type=F32)
        total = None
        for m in range(members):
            term = pert_of(blocks, k * members + m) * field[:, m * TILE : (m + 1) * TILE]
            total = term if total is None else total + term
        total = total.astype(BF16)
        for h in range(8):
            cells_ref[k, chip_of(place_ref, h)] = total[h * 32 : (h + 1) * 32]
        stores.append(pltpu.make_async_copy(cells_ref.at[k], cells_hbm.at[k], writes.at[k]))
        stores[-1].start()
        turned = jnp.transpose(tiles.astype(F32)).astype(BF16)
        for q in range(2):
            for l in range(2):
                at = (2 * l + q) * rows
                turned_ref[k, (2 * q + l) * rows : (2 * q + l + 1) * rows, :] = turned[at : at + rows]
    stores.append(pltpu.make_async_copy(turned_ref, turned_hbm, writes.at[8]))
    stores[-1].start()
    for store in stores:
        store.wait()


def score(cells_ref, own_ref, lent_ref, out_ref):
    copies = out_ref.shape[0]
    total = jnp.sum(cells_ref[...].astype(F32), axis=0)
    value = jnp.concatenate([own_ref[0], lent_ref[0]], axis=0)
    seen = jnp.concatenate([own_ref[1], lent_ref[1]], axis=0)
    resid = total - value
    result = jnp.where(seen > 0.5, resid / jnp.sqrt(1.0 + resid * resid * 0.25), 0.0)
    result = result.astype(BF16)
    for i in range(copies):
        out_ref[i] = result


def back(place_ref, *refs):
    blocks, (score_ref, turned_hbm, own_ref, par_ref, turned, sem) = refs[:8], refs[8:]
    members, depth, _ = own_ref.shape
    load = pltpu.make_async_copy(turned_hbm, turned, sem)
    load.start()
    for k in range(8):
        weight = jnp.concatenate(
            [score_ref[k, chip_of(place_ref, h)] for h in range(8)], axis=0
        ).astype(F32)
        weighted = jnp.concatenate(
            [(pert_of(blocks, k * members + m) * weight).astype(BF16) for m in range(members)],
            axis=1,
        )
        if k == 0:
            load.wait()
        result = jnp.dot(turned[k], weighted, preferred_element_type=F32).astype(BF16)
        for m in range(members):
            part = result[:, m * TILE : (m + 1) * TILE]
            own_ref[m, :, k * TILE : (k + 1) * TILE] = part[:depth]
            par_ref[m, :, k * TILE : (k + 1) * TILE] = part[depth:]


def streamed(tables, rows, block_ref, sems):
    steps = tables[0].shape[0]

    def fetch(i, n, slot):
        return pltpu.make_async_copy(tables[i].at[n, rows, :], block_ref.at[slot], sems.at[slot])

    def at(i, n):
        slot = lax.rem(n, 2)

        @pl.when(n + 1 < steps)
        def _():
            fetch(i, n + 1, 1 - slot).start()

        if i + 1 < len(tables):

            @pl.when(n + 1 == steps)
            def _():
                fetch(i + 1, 0, 1 - slot).start()

        fetch(i, n, slot).wait()
        return block_ref[slot]

    fetch(0, 0, 0).start()
    return at


def inverse_own(core_ref, own_ref, table0_ref, table1_ref, sum_ref, block_ref, sems):
    members, depth, width = own_ref.shape
    near = pl.ds(pl.multiple_of(core_ref[0] * width, width), width)
    half = table0_ref.shape[0]
    core = core_ref[0]
    block = streamed((table0_ref, table1_ref), near, block_ref, sems)
    for i in range(2):
        which = (1 - core) if i == 0 else core

        def step(n, carry, i=i, which=which):
            sum_ref[which * half + n] = jnp.dot(
                own_ref[...].reshape(members * depth, width),
                block(i, n),
                preferred_element_type=F32,
            )
            return carry

        lax.fori_loop(0, half, step, 0)


def inverse_par(
    core_ref, par_ref, sum_ref, table0_ref, table1_ref, row_ref, col_ref, out_ref,
    piece, sems, block_ref, reads,
):
    members, depth, width = par_ref.shape
    levels, rows, _ = row_ref.shape
    core = core_ref[0]
    half = table0_ref.shape[0]
    far = pl.ds(pl.multiple_of((1 - core) * width, width), width)

    def copy(nb, slot):
        cols = pl.ds(pl.multiple_of(nb * WIDE, WIDE), WIDE)
        return pltpu.make_async_copy(piece.at[slot], out_ref.at[:, :, :, cols], sems.at[slot])

    block = streamed((table0_ref, table1_ref), far, block_ref, reads)
    for i in range(2):
        which = (1 - core) if i == 0 else core

        def step(n, carry, i=i, which=which):
            slot = lax.rem(n, 2)
            nb = which * half + n
            cols = pl.ds(pl.multiple_of(nb * WIDE, WIDE), WIDE)
            product = sum_ref[nb] + jnp.dot(
                par_ref[...].reshape(members * depth, width),
                block(i, n),
                preferred_element_type=F32,
            )
            product = product.reshape(members, levels, rows, WIDE)

            @pl.when(n >= (2 if i == 0 else 0))
            def _():
                copy(nb, slot).wait()

            for l in range(levels):
                amplitude = row_ref[l][:, :1] * col_ref[l : l + 1, cols]
                for m in range(members):
                    piece[slot, m, l] = product[m, l] * amplitude
            copy(nb, slot).start()
            return carry

        lax.fori_loop(0, half, step, 0)
    for slot in range(2):
        copy(slot, slot).wait()


def shards(control, perturbation, loc_row, loc_col, obs_tile, obs_count, obs_value):
    members, levels, rows, width = control.shape
    slabs = 16
    peers = lax.axis_size("member") * 8
    height = rows * slabs
    half = width // 2
    per_core = half // TILE
    depth = levels * rows
    across = lax.axis_index("across").astype(jnp.int32)
    along = lax.axis_index("along").astype(jnp.int32)
    core = lax.axis_index("core").astype(jnp.int32)
    group = lax.axis_index("member").astype(jnp.int32)
    core_index = core.reshape(1)
    place = jnp.stack([across, along, core])
    swap = [(0, 1), (1, 0)]

    def from_next(array, step):
        return lax.ppermute(array, "along", [((i + step) % 4, i) for i in range(4)])

    blocks = per_core * members + 1
    own_tiles, send_tiles = run(
        select,
        [bf16(blocks, 16, TILE)] * 2,
        [SMEM, HBM, HBM],
        1 << 27,
        [
            pltpu.VMEM((2, TILE), jnp.int32),
            pltpu.VMEM(perturbation.shape, BF16),
            pltpu.SemaphoreType.DMA((members + 1,)),
        ],
    )(core_index, obs_tile.reshape(2, TILE), perturbation)
    here = jnp.stack([own_tiles, lax.ppermute(send_tiles, "core", swap)])
    facing = lax.ppermute(here, "across", swap)
    here2 = from_next(here, 2)
    here1, here3 = from_next(here, 1), from_next(here, 3)
    facing1, facing3 = from_next(facing, 1), from_next(facing, 3)
    facing2 = lax.ppermute(here2, "across", swap)
    arrived = (here, here1, here2, here3, facing, facing1, facing2, facing3)

    lane = jnp.arange(TILE, dtype=jnp.int32)

    def of_column(column, array):
        return lax.dynamic_slice_in_dim(array, column * 16, 16, 0)

    seen = (lane[None, :] < obs_count[:, None]).astype(F32)
    mine = per_core * core + group
    other = per_core * (1 - core) + group
    stated = jnp.stack([of_column(mine, obs_value), of_column(mine, seen)])
    lent = jnp.stack([of_column(other, obs_value), of_column(other, seen)])
    lent = lax.ppermute(lent, "core", swap)

    lead = cas(np.arange(16), np.arange(16), 16)
    lead = jnp.asarray(np.repeat(np.stack(lead[2:])[:, :, :, None], TILE, axis=3))
    inner = 64
    outer = cas(np.arange(width // inner), np.arange(TILE), width // inner)
    near = cas(np.arange(inner), np.arange(TILE), width)
    root = np.float32(np.sqrt(width))
    factors = jnp.asarray(np.concatenate([outer[2], outer[3], near[0] / root, near[1] / root]))
    wave = np.arange(TILE) % rows
    base = cas(np.arange(rows), wave, height)
    turn = cas(np.arange(16), wave, 16)
    root = np.float32(np.sqrt(height))
    row_factors = jnp.asarray(np.concatenate([base[0] / root, base[1] / root, turn[2], turn[3]]))

    row_b = jnp.broadcast_to(loc_row[:, :, None], (levels, rows, TILE))
    table_half = bf16(width // WIDE // 2, width, WIDE)
    work = [
        pltpu.VMEM((width, TILE), F32),
        pltpu.VMEM((width, TILE), F32),
        pltpu.VMEM((2, width, WIDE), BF16),
        pltpu.SemaphoreType.DMA((2,)),
    ]
    flops = members * depth * width * width
    send, scaled, table0 = run(
        forward_send,
        [bf16(members, depth, half), bf16(members * depth, width), table_half],
        [SMEM, HBM, VMEM, VMEM, VMEM, VMEM, HBM],
        flops,
        [pltpu.VMEM(control.shape, F32)] + work + [pltpu.SemaphoreType.DMA((members,))],
        [VMEM, VMEM, HBM],
    )(core_index, control, row_b, loc_col, factors, lead, here)
    par = lax.ppermute(send, "core", swap)
    own, table1 = run(
        forward_own,
        [bf16(members, depth, half), table_half],
        [SMEM, VMEM, VMEM, VMEM, HBM, HBM],
        flops,
        work,
        [VMEM, HBM],
    )(core_index, scaled, factors, lead, facing, here2)
    table_rows = run(
        spread_rows, bf16(8, 4 * rows, 2 * TILE), [SMEM, VMEM, VMEM], 1 << 22
    )(place, row_factors, lead)

    tiles = slabs * 16
    partial, turned = run(
        cells,
        [bf16(per_core, 8, 2 * 16, TILE), bf16(per_core, 4 * rows, tiles)],
        [SMEM] + [VMEM] * 8 + [HBM, HBM, VMEM],
        1 << 30,
        [
            pltpu.VMEM((members, depth, half), BF16),
            pltpu.VMEM((members, depth, half), BF16),
            pltpu.VMEM((8, tiles, 4 * rows), BF16),
            pltpu.VMEM((per_core, 8, 2 * 16, TILE), BF16),
            pltpu.VMEM((per_core, 4 * rows, tiles), BF16),
            pltpu.SemaphoreType.DMA((2,)),
            pltpu.SemaphoreType.DMA((9,)),
        ],
        [HBM, HBM],
    )(place, *arrived, own, par, table_rows)
    partial = lax.all_to_all(
        partial.reshape(peers, 2 * 16, TILE), SAME_CORE, split_axis=0, concat_axis=0, tiled=True
    )
    scores = run(score, bf16(peers, 2 * 16, TILE), [VMEM] * 3, 1 << 20)(partial, stated, lent)
    scores = lax.all_to_all(scores, SAME_CORE, split_axis=0, concat_axis=0, tiled=True)

    back_own, back_send = run(
        back,
        [bf16(members, depth, half)] * 2,
        [SMEM] + [VMEM] * 9 + [HBM],
        1 << 28,
        [pltpu.VMEM((per_core, 4 * rows, tiles), BF16), pltpu.SemaphoreType.DMA],
        mib=58,
    )(place, *arrived, scores.reshape(per_core, 8, 2 * 16, TILE), turned)
    back_other = lax.ppermute(back_send, "core", swap)
    stream = [pltpu.VMEM((2, half, WIDE), BF16), pltpu.SemaphoreType.DMA((2,))]
    summed = run(
        inverse_own,
        f32(width // WIDE, members * depth, WIDE),
        [SMEM, VMEM, HBM, HBM],
        flops,
        stream,
        mib=54,
    )(core_index, back_own, table0, table1)
    return run(
        inverse_par,
        f32(*control.shape),
        [SMEM, VMEM, VMEM, HBM, HBM, VMEM, VMEM],
        flops,
        [pltpu.VMEM((2, members, levels, rows, WIDE), F32), pltpu.SemaphoreType.DMA((2,))] + stream,
        [HBM],
        mib=54,
    )(core_index, back_other, summed, table0, table1, row_b, loc_col)


def solution(mesh):
    torus = Mesh(
        mesh.devices.reshape(mesh.shape["member"], 2, 4, 2),
        ("member", "across", "along", "core"),
    )
    placed = (
        P("member", None, SLAB, None),
        P("member", None, SLAB, None),
        P(None, SLAB),
        P(),
        P(SLAB),
        P(SLAB),
        P(SLAB, None),
    )
    return jax.shard_map(
        shards,
        mesh=torus,
        in_specs=placed,
        out_specs=P("member", None, SLAB, None),
        check_vma=False,
    )
```

```python
import jax
import jax.numpy as jnp
import numpy as np
from jax import lax
from jax.experimental import pallas as pl
from jax.experimental.pallas import tpu as pltpu
from jax.sharding import Mesh
from jax.sharding import PartitionSpec as P

TILE = 128
WIDE = 256
BF16 = jnp.bfloat16
F32 = jnp.float32
SLAB = ("across", "along", "core")
SAME_CORE = ("member", "across", "along")
VMEM = pl.BlockSpec(memory_space=pltpu.VMEM)
SMEM = pl.BlockSpec(memory_space=pltpu.SMEM)
HBM = pl.BlockSpec(memory_space=pltpu.HBM)


def run(kernel, out_shape, in_specs, flops, scratch=(), out_specs=None, mib=24):
    outs = out_shape if isinstance(out_shape, list) else [out_shape]
    if out_specs is None:
        out_specs = [VMEM] * len(outs)
    moved = sum(int(np.prod(o.shape)) * o.dtype.itemsize for o in outs) * 2
    call = pl.pallas_call(
        kernel,
        in_specs=in_specs,
        out_specs=out_specs,
        out_shape=outs,
        scratch_shapes=list(scratch),
        compiler_params=pltpu.CompilerParams(vmem_limit_bytes=mib << 20),
        cost_estimate=pl.CostEstimate(flops=flops, bytes_accessed=moved, transcendentals=0),
    )

    def launch(*args):
        results = call(*args)
        return results if isinstance(out_shape, list) else results[0]

    return launch


def bf16(*shape):
    return jax.ShapeDtypeStruct(shape, BF16)


def f32(*shape):
    return jax.ShapeDtypeStruct(shape, F32)


def cas(first, second, order):
    angle = 2.0 * np.pi * (np.outer(first, second) % order) / order
    c, s = np.cos(angle), np.sin(angle)
    return [a.astype(np.float32) for a in (c + s, c - s, c, s)]


def select(core_ref, tile_ref, pert_ref, own_ref, send_ref, tiles, pert, sems):
    members = pert.shape[0]
    core = core_ref[0]
    copies = [pltpu.make_async_copy(tile_ref, tiles, sems.at[members])]
    copies += [pltpu.make_async_copy(pert_ref.at[m], pert.at[m], sems.at[m]) for m in range(members)]
    for copy in copies:
        copy.start()
    copies[0].wait()
    place = tiles[...] // 16
    row = lax.broadcasted_iota(jnp.int32, (TILE, TILE), 0)
    halves = []
    for half in (1 - core, core):
        mine = jnp.where(half == 0, place[0:1, :], place[1:2, :])
        halves.append((mine, jnp.transpose((row == mine).astype(F32)).astype(BF16)))
    for copy in copies[1:]:
        copy.wait()
    for ref, half, (mine, chosen) in zip((send_ref, own_ref), (1 - core, core), halves):
        for k in range(8):
            cols = pl.ds(pl.multiple_of((half * 8 + k) * TILE, TILE), TILE)
            tile = jnp.concatenate(
                [pert[m, :, :, cols].reshape(TILE, TILE) for m in range(members)], axis=1
            )
            rows = jnp.dot(
                chosen[16 * k : 16 * k + 16], tile, preferred_element_type=F32
            ).astype(BF16)
            for m in range(members):
                ref[k * members + m] = rows[:, m * TILE : (m + 1) * TILE]
        ref[8 * members] = jnp.broadcast_to(mine.astype(F32), (16, TILE)).astype(BF16)


def table_factors(factor_ref, width, plus, minus):
    inner = 64
    outer = width // inner
    near_p = factor_ref[2 * outer : 2 * outer + inner, :]
    near_m = factor_ref[2 * outer + inner : 2 * outer + 2 * inner, :]
    for u in range(outer):
        at = slice(u * inner, (u + 1) * inner)
        c, s = factor_ref[u : u + 1, :], factor_ref[outer + u : outer + u + 1, :]
        plus[at, :] = c * near_p + s * near_m
        minus[at, :] = c * near_m - s * near_p


def transform(which, scaled, lead_ref, plus, minus, block_ref, table_ref, sems, target):
    width = plus.shape[0]
    members, depth, _ = target.shape
    half = width // WIDE // 2

    def copy(nb, slot):
        return pltpu.make_async_copy(block_ref.at[slot], table_ref.at[nb], sems.at[slot])

    def step(n, carry):
        nb = which * half + n
        slot = lax.rem(n, 2)

        @pl.when(n >= 2)
        def _():
            copy(n - 2, slot).wait()

        for q in range(WIDE // TILE):
            c = lead_ref[0, nb * (WIDE // TILE) + q]
            s = lead_ref[1, nb * (WIDE // TILE) + q]
            c = jnp.broadcast_to(c[None], (width // 16, 16, TILE)).reshape(width, TILE)
            s = jnp.broadcast_to(s[None], (width // 16, 16, TILE)).reshape(width, TILE)
            block_ref[slot, :, q * TILE : (q + 1) * TILE] = (
                c * plus[...] + s * minus[...]
            ).astype(BF16)
        copy(n, slot).start()
        product = jnp.dot(scaled[...], block_ref[slot], preferred_element_type=F32)
        to = pl.ds(pl.multiple_of(n * WIDE, WIDE), WIDE)
        target[:, :, to] = product.astype(BF16).reshape(members, depth, WIDE)
        return carry

    lax.fori_loop(0, half, step, 0)
    for slot in range(2):
        copy(slot, slot).wait()


def forward_send(
    core_ref, control_ref, row_ref, col_ref, factor_ref, lead_ref, after_ref,
    send_ref, scaled_ref, table_ref,
    control, plus, minus, block_ref, sems, reads,
):
    members, levels, rows, width = control.shape
    copies = [
        pltpu.make_async_copy(control_ref.at[m], control.at[m], reads.at[m]) for m in range(members)
    ]
    for copy in copies:
        copy.start()
    table_factors(factor_ref, width, plus, minus)
    for m in range(members):
        copies[m].wait()
        for l in range(levels):
            amplitude = row_ref[l][:, :1] * col_ref[l : l + 1, :]
            at = (m * levels + l) * rows
            scaled_ref[at : at + rows, :] = (control[m, l] * amplitude).astype(BF16)
    transform(
        1 - core_ref[0], scaled_ref, lead_ref, plus, minus, block_ref, table_ref, sems, send_ref
    )


def forward_own(
    core_ref, scaled_ref, factor_ref, lead_ref, after0_ref, after1_ref,
    own_ref, table_ref, plus, minus, block_ref, sems,
):
    table_factors(factor_ref, plus.shape[0], plus, minus)
    transform(core_ref[0], scaled_ref, lead_ref, plus, minus, block_ref, table_ref, sems, own_ref)


def chip_of(place_ref, h):
    across, along = place_ref[0], place_ref[1]
    return ((across + h // 4) % 2) * 4 + (along + h % 4) % 4


def spread_rows(place_ref, factor_ref, lead_ref, out_ref):
    core = place_ref[2]
    rows = out_ref.shape[1] // 4
    inner_p, inner_m = factor_ref[:rows, :], factor_ref[rows : 2 * rows, :]
    plus, minus = [], []
    for q in range(2):
        slab = chip_of(place_ref, 0) * 2 + (core + q) % 2
        c = jnp.broadcast_to(lead_ref[0, slab][None], (rows // 16, 16, TILE)).reshape(rows, TILE)
        s = jnp.broadcast_to(lead_ref[1, slab][None], (rows // 16, 16, TILE)).reshape(rows, TILE)
        plus.append(c * inner_p + s * inner_m)
        minus.append(c * inner_m - s * inner_p)
    left = lax.broadcasted_iota(jnp.int32, (rows, TILE), 1) < rows
    plus = jnp.where(left, plus[0], plus[1])
    minus = jnp.where(left, minus[0], minus[1])
    nothing = jnp.zeros((rows, TILE), BF16)
    for h in range(out_ref.shape[0]):
        for r in range(2):
            slab = chip_of(place_ref, h) * 2 + (core + r) % 2
            c = factor_ref[pl.ds(2 * rows + slab, 1), :]
            s = factor_ref[pl.ds(2 * rows + 16 + slab, 1), :]
            entry = (c * plus + s * minus).astype(BF16)
            for l in range(2):
                at = slice((2 * l + r) * rows, (2 * l + r + 1) * rows)
                out_ref[h, at, l * TILE : (l + 1) * TILE] = entry
                out_ref[h, at, (1 - l) * TILE : (2 - l) * TILE] = nothing


def pert_of(blocks, at):
    return jnp.concatenate([ref[:, at].reshape(-1, TILE) for ref in blocks], axis=0).astype(F32)


def cells(place_ref, *refs):
    blocks, (own_hbm, par_hbm, rows_ref, cells_hbm, turned_hbm) = refs[:8], refs[8:13]
    own, par, spread, cells_ref, turned_ref, reads, writes = refs[13:]
    members, depth, _ = own.shape
    rows = depth // 2
    last = blocks[0].shape[1] - 1
    loads = [
        pltpu.make_async_copy(own_hbm, own, reads.at[0]),
        pltpu.make_async_copy(par_hbm, par, reads.at[1]),
    ]
    for load in loads:
        load.start()
    lane = lax.broadcasted_iota(jnp.int32, (1, 2 * TILE), 1)
    row = lax.broadcasted_iota(jnp.int32, (4 * rows, 2 * TILE), 0)
    for h, block in enumerate(blocks):
        place = jnp.concatenate(
            [block[r, last].astype(F32)[0:1, :] for r in range(2)], axis=1
        ).astype(jnp.int32)
        level, inside = place // rows, place % rows
        place = level * (2 * rows) + inside + jnp.where(lane < TILE, 0, rows)
        chosen = (row == place).astype(F32).astype(BF16)
        spread[h] = lax.dot_general(
            chosen, rows_ref[h], (((0,), (0,)), ((), ())), preferred_element_type=F32
        ).astype(BF16)
    for load in loads:
        load.wait()
    stores = []
    for k in range(8):
        cols = slice(k * TILE, (k + 1) * TILE)
        along = jnp.concatenate(
            [
                jnp.concatenate(
                    [ref[m, l * rows : (l + 1) * rows, cols] for m in range(members)], axis=1
                )
                for l in range(2)
                for ref in (own, par)
            ],
            axis=0,
        )
        tiles = jnp.concatenate(
            [
                spread[h, r * TILE + k * 16 : r * TILE + (k + 1) * 16, :]
                for h in range(8)
                for r in range(2)
            ],
            axis=0,
        )
        field = jnp.dot(tiles, along, preferred_element_type=F32)
        total = None
        for m in range(members):
            term = pert_of(blocks, k * members + m) * field[:, m * TILE : (m + 1) * TILE]
            total = term if total is None else total + term
        total = total.astype(BF16)
        for h in range(8):
            cells_ref[k, chip_of(place_ref, h)] = total[h * 32 : (h + 1) * 32]
        stores.append(pltpu.make_async_copy(cells_ref.at[k], cells_hbm.at[k], writes.at[k]))
        stores[-1].start()
        turned = jnp.transpose(tiles.astype(F32)).astype(BF16)
        for q in range(2):
            for l in range(2):
                at = (2 * l + q) * rows
                turned_ref[k, (2 * q + l) * rows : (2 * q + l + 1) * rows, :] = turned[at : at + rows]
    stores.append(pltpu.make_async_copy(turned_ref, turned_hbm, writes.at[8]))
    stores[-1].start()
    for store in stores:
        store.wait()


def score(cells_ref, own_ref, lent_ref, out_ref):
    copies = out_ref.shape[0]
    total = jnp.sum(cells_ref[...].astype(F32), axis=0)
    value = jnp.concatenate([own_ref[0], lent_ref[0]], axis=0)
    seen = jnp.concatenate([own_ref[1], lent_ref[1]], axis=0)
    resid = total - value
    result = jnp.where(seen > 0.5, resid / jnp.sqrt(1.0 + resid * resid * 0.25), 0.0)
    result = result.astype(BF16)
    for i in range(copies):
        out_ref[i] = result


def back(place_ref, *refs):
    blocks, (score_ref, turned_hbm, own_ref, par_ref, turned, sem) = refs[:8], refs[8:]
    members, depth, _ = own_ref.shape
    load = pltpu.make_async_copy(turned_hbm, turned, sem)
    load.start()
    for k in range(8):
        weight = jnp.concatenate(
            [score_ref[k, chip_of(place_ref, h)] for h in range(8)], axis=0
        ).astype(F32)
        weighted = jnp.concatenate(
            [(pert_of(blocks, k * members + m) * weight).astype(BF16) for m in range(members)],
            axis=1,
        )
        if k == 0:
            load.wait()
        result = jnp.dot(turned[k], weighted, preferred_element_type=F32).astype(BF16)
        for m in range(members):
            part = result[:, m * TILE : (m + 1) * TILE]
            own_ref[m, :, k * TILE : (k + 1) * TILE] = part[:depth]
            par_ref[m, :, k * TILE : (k + 1) * TILE] = part[depth:]


def streamed(tables, rows, block_ref, sems):
    steps = tables[0].shape[0]

    def fetch(i, n):
        at = i * steps + n
        return pltpu.make_async_copy(tables[i].at[n, rows, :], block_ref.at[at], sems.at[at])

    for i in range(len(tables)):
        for n in range(steps):
            fetch(i, n).start()

    def block(i, n):
        fetch(i, n).wait()
        return block_ref[i * steps + n]

    return block


def inverse_own(core_ref, own_ref, table0_ref, table1_ref, sum_ref, block_ref, sems):
    members, depth, width = own_ref.shape
    near = pl.ds(pl.multiple_of(core_ref[0] * width, width), width)
    half = table0_ref.shape[0]
    core = core_ref[0]
    block = streamed((table0_ref, table1_ref), near, block_ref, sems)
    for i in range(2):
        which = (1 - core) if i == 0 else core

        def step(n, carry, i=i, which=which):
            sum_ref[which * half + n] = jnp.dot(
                own_ref[...].reshape(members * depth, width),
                block(i, n),
                preferred_element_type=F32,
            )
            return carry

        lax.fori_loop(0, half, step, 0)


def inverse_par(
    core_ref, par_ref, sum_ref, table0_ref, table1_ref, row_ref, col_ref, out_ref,
    piece, sems, block_ref, reads,
):
    members, depth, width = par_ref.shape
    levels, rows, _ = row_ref.shape
    core = core_ref[0]
    half = table0_ref.shape[0]
    far = pl.ds(pl.multiple_of((1 - core) * width, width), width)

    def copy(nb, slot):
        cols = pl.ds(pl.multiple_of(nb * WIDE, WIDE), WIDE)
        return pltpu.make_async_copy(piece.at[slot], out_ref.at[:, :, :, cols], sems.at[slot])

    block = streamed((table0_ref, table1_ref), far, block_ref, reads)
    for i in range(2):
        which = (1 - core) if i == 0 else core

        def step(n, carry, i=i, which=which):
            slot = lax.rem(n, 2)
            nb = which * half + n
            cols = pl.ds(pl.multiple_of(nb * WIDE, WIDE), WIDE)
            product = sum_ref[nb] + jnp.dot(
                par_ref[...].reshape(members * depth, width),
                block(i, n),
                preferred_element_type=F32,
            )
            product = product.reshape(members, levels, rows, WIDE)

            @pl.when(n >= (2 if i == 0 else 0))
            def _():
                copy(nb, slot).wait()

            for l in range(levels):
                amplitude = row_ref[l][:, :1] * col_ref[l : l + 1, cols]
                for m in range(members):
                    piece[slot, m, l] = product[m, l] * amplitude
            copy(nb, slot).start()
            return carry

        lax.fori_loop(0, half, step, 0)
    for slot in range(2):
        copy(slot, slot).wait()


def shards(control, perturbation, loc_row, loc_col, obs_tile, obs_count, obs_value):
    members, levels, rows, width = control.shape
    slabs = 16
    peers = lax.axis_size("member") * 8
    height = rows * slabs
    half = width // 2
    per_core = half // TILE
    depth = levels * rows
    across = lax.axis_index("across").astype(jnp.int32)
    along = lax.axis_index("along").astype(jnp.int32)
    core = lax.axis_index("core").astype(jnp.int32)
    group = lax.axis_index("member").astype(jnp.int32)
    core_index = core.reshape(1)
    place = jnp.stack([across, along, core])
    swap = [(0, 1), (1, 0)]

    def from_next(array, step):
        return lax.ppermute(array, "along", [((i + step) % 4, i) for i in range(4)])

    blocks = per_core * members + 1
    own_tiles, send_tiles = run(
        select,
        [bf16(blocks, 16, TILE)] * 2,
        [SMEM, HBM, HBM],
        1 << 27,
        [
            pltpu.VMEM((2, TILE), jnp.int32),
            pltpu.VMEM(perturbation.shape, BF16),
            pltpu.SemaphoreType.DMA((members + 1,)),
        ],
    )(core_index, obs_tile.reshape(2, TILE), perturbation)
    here = jnp.stack([own_tiles, lax.ppermute(send_tiles, "core", swap)])
    facing = lax.ppermute(here, "across", swap)
    here2 = from_next(here, 2)
    here1, here3 = from_next(here, 1), from_next(here, 3)
    facing1, facing3 = from_next(facing, 1), from_next(facing, 3)
    facing2 = lax.ppermute(here2, "across", swap)
    arrived = (here, here1, here2, here3, facing, facing1, facing2, facing3)

    lane = jnp.arange(TILE, dtype=jnp.int32)

    def of_column(column, array):
        return lax.dynamic_slice_in_dim(array, column * 16, 16, 0)

    seen = (lane[None, :] < obs_count[:, None]).astype(F32)
    mine = per_core * core + group
    other = per_core * (1 - core) + group
    stated = jnp.stack([of_column(mine, obs_value), of_column(mine, seen)])
    lent = jnp.stack([of_column(other, obs_value), of_column(other, seen)])
    lent = lax.ppermute(lent, "core", swap)

    lead = cas(np.arange(16), np.arange(16), 16)
    lead = jnp.asarray(np.repeat(np.stack(lead[2:])[:, :, :, None], TILE, axis=3))
    inner = 64
    outer = cas(np.arange(width // inner), np.arange(TILE), width // inner)
    near = cas(np.arange(inner), np.arange(TILE), width)
    root = np.float32(np.sqrt(width))
    factors = jnp.asarray(np.concatenate([outer[2], outer[3], near[0] / root, near[1] / root]))
    wave = np.arange(TILE) % rows
    base = cas(np.arange(rows), wave, height)
    turn = cas(np.arange(16), wave, 16)
    root = np.float32(np.sqrt(height))
    row_factors = jnp.asarray(np.concatenate([base[0] / root, base[1] / root, turn[2], turn[3]]))

    row_b = jnp.broadcast_to(loc_row[:, :, None], (levels, rows, TILE))
    table_half = bf16(width // WIDE // 2, width, WIDE)
    work = [
        pltpu.VMEM((width, TILE), F32),
        pltpu.VMEM((width, TILE), F32),
        pltpu.VMEM((2, width, WIDE), BF16),
        pltpu.SemaphoreType.DMA((2,)),
    ]
    flops = members * depth * width * width
    send, scaled, table0 = run(
        forward_send,
        [bf16(members, depth, half), bf16(members * depth, width), table_half],
        [SMEM, HBM, VMEM, VMEM, VMEM, VMEM, HBM],
        flops,
        [pltpu.VMEM(control.shape, F32)] + work + [pltpu.SemaphoreType.DMA((members,))],
        [VMEM, VMEM, HBM],
        mib=48,
    )(core_index, control, row_b, loc_col, factors, lead, here)
    par = lax.ppermute(send, "core", swap)
    own, table1 = run(
        forward_own,
        [bf16(members, depth, half), table_half],
        [SMEM, VMEM, VMEM, VMEM, HBM, HBM],
        flops,
        work,
        [VMEM, HBM],
        mib=48,
    )(core_index, scaled, factors, lead, facing, here2)
    table_rows = run(
        spread_rows, bf16(8, 4 * rows, 2 * TILE), [SMEM, VMEM, VMEM], 1 << 22
    )(place, row_factors, lead)

    tiles = slabs * 16
    partial, turned = run(
        cells,
        [bf16(per_core, 8, 2 * 16, TILE), bf16(per_core, 4 * rows, tiles)],
        [SMEM] + [VMEM] * 8 + [HBM, HBM, VMEM],
        1 << 30,
        [
            pltpu.VMEM((members, depth, half), BF16),
            pltpu.VMEM((members, depth, half), BF16),
            pltpu.VMEM((8, tiles, 4 * rows), BF16),
            pltpu.VMEM((per_core, 8, 2 * 16, TILE), BF16),
            pltpu.VMEM((per_core, 4 * rows, tiles), BF16),
            pltpu.SemaphoreType.DMA((2,)),
            pltpu.SemaphoreType.DMA((9,)),
        ],
        [HBM, HBM],
    )(place, *arrived, own, par, table_rows)
    partial = lax.all_to_all(
        partial.reshape(peers, 2 * 16, TILE), SAME_CORE, split_axis=0, concat_axis=0, tiled=True
    )
    scores = run(score, bf16(peers, 2 * 16, TILE), [VMEM] * 3, 1 << 20)(partial, stated, lent)
    scores = lax.all_to_all(scores, SAME_CORE, split_axis=0, concat_axis=0, tiled=True)

    back_own, back_send = run(
        back,
        [bf16(members, depth, half)] * 2,
        [SMEM] + [VMEM] * 9 + [HBM],
        1 << 28,
        [pltpu.VMEM((per_core, 4 * rows, tiles), BF16), pltpu.SemaphoreType.DMA],
        mib=24,
    )(place, *arrived, scores.reshape(per_core, 8, 2 * 16, TILE), turned)
    back_other = lax.ppermute(back_send, "core", swap)
    parts = width // WIDE
    stream = [pltpu.VMEM((parts, half, WIDE), BF16), pltpu.SemaphoreType.DMA((parts,))]
    summed = run(
        inverse_own,
        f32(width // WIDE, members * depth, WIDE),
        [SMEM, VMEM, HBM, HBM],
        flops,
        stream,
        mib=46,
    )(core_index, back_own, table0, table1)
    return run(
        inverse_par,
        f32(*control.shape),
        [SMEM, VMEM, VMEM, HBM, HBM, VMEM, VMEM],
        flops,
        [pltpu.VMEM((2, members, levels, rows, WIDE), F32), pltpu.SemaphoreType.DMA((2,))] + stream,
        [HBM],
        mib=46,
    )(core_index, back_other, summed, table0, table1, row_b, loc_col)


def solution(mesh):
    torus = Mesh(
        mesh.devices.reshape(mesh.shape["member"], 2, 4, 2),
        ("member", "across", "along", "core"),
    )
    placed = (
        P("member", None, SLAB, None),
        P("member", None, SLAB, None),
        P(None, SLAB),
        P(),
        P(SLAB),
        P(SLAB),
        P(SLAB, None),
    )
    return jax.shard_map(
        shards,
        mesh=torus,
        in_specs=placed,
        out_specs=P("member", None, SLAB, None),
        check_vma=False,
    )
```

```python
import jax
import jax.numpy as jnp
import numpy as np
from jax import lax
from jax.experimental import pallas as pl
from jax.experimental.pallas import tpu as pltpu
from jax.sharding import Mesh
from jax.sharding import PartitionSpec as P

TILE = 128
WIDE = 256
BF16 = jnp.bfloat16
F32 = jnp.float32
SLAB = ("across", "along", "core")
SAME_CORE = ("member", "across", "along")
VMEM = pl.BlockSpec(memory_space=pltpu.VMEM)
SMEM = pl.BlockSpec(memory_space=pltpu.SMEM)
HBM = pl.BlockSpec(memory_space=pltpu.HBM)


def run(kernel, out_shape, in_specs, flops, scratch=(), out_specs=None, mib=46):
    outs = out_shape if isinstance(out_shape, list) else [out_shape]
    if out_specs is None:
        out_specs = [VMEM] * len(outs)
    moved = sum(int(np.prod(o.shape)) * o.dtype.itemsize for o in outs) * 2
    call = pl.pallas_call(
        kernel,
        in_specs=in_specs,
        out_specs=out_specs,
        out_shape=outs,
        scratch_shapes=list(scratch),
        compiler_params=pltpu.CompilerParams(vmem_limit_bytes=mib << 20),
        cost_estimate=pl.CostEstimate(flops=flops, bytes_accessed=moved, transcendentals=0),
    )

    def launch(*args):
        results = call(*args)
        return results if isinstance(out_shape, list) else results[0]

    return launch


def bf16(*shape):
    return jax.ShapeDtypeStruct(shape, BF16)


def f32(*shape):
    return jax.ShapeDtypeStruct(shape, F32)


def cas(first, second, order):
    angle = 2.0 * np.pi * (np.outer(first, second) % order) / order
    c, s = np.cos(angle), np.sin(angle)
    return [a.astype(np.float32) for a in (c + s, c - s, c, s)]


def select(core_ref, tile_ref, pert_ref, own_ref, send_ref, tiles, pert, sems):
    members = pert.shape[0]
    core = core_ref[0]
    copies = [pltpu.make_async_copy(tile_ref, tiles, sems.at[members])]
    copies += [pltpu.make_async_copy(pert_ref.at[m], pert.at[m], sems.at[m]) for m in range(members)]
    for copy in copies:
        copy.start()
    copies[0].wait()
    place = tiles[...] // 16
    row = lax.broadcasted_iota(jnp.int32, (TILE, TILE), 0)
    halves = []
    for half in (1 - core, core):
        mine = jnp.where(half == 0, place[0:1, :], place[1:2, :])
        halves.append((mine, jnp.transpose((row == mine).astype(F32)).astype(BF16)))
    for copy in copies[1:]:
        copy.wait()
    for ref, half, (mine, chosen) in zip((send_ref, own_ref), (1 - core, core), halves):
        for k in range(8):
            cols = pl.ds(pl.multiple_of((half * 8 + k) * TILE, TILE), TILE)
            tile = jnp.concatenate(
                [pert[m, :, :, cols].reshape(TILE, TILE) for m in range(members)], axis=1
            )
            rows = jnp.dot(
                chosen[16 * k : 16 * k + 16], tile, preferred_element_type=F32
            ).astype(BF16)
            for m in range(members):
                ref[k * members + m] = rows[:, m * TILE : (m + 1) * TILE]
        ref[8 * members] = jnp.broadcast_to(mine.astype(F32), (16, TILE)).astype(BF16)


def table_factors(factor_ref, width, plus, minus):
    inner = 64
    outer = width // inner
    near_p = factor_ref[2 * outer : 2 * outer + inner, :]
    near_m = factor_ref[2 * outer + inner : 2 * outer + 2 * inner, :]
    for u in range(outer):
        at = slice(u * inner, (u + 1) * inner)
        c, s = factor_ref[u : u + 1, :], factor_ref[outer + u : outer + u + 1, :]
        plus[at, :] = c * near_p + s * near_m
        minus[at, :] = c * near_m - s * near_p


def transform(which, scaled, lead_ref, plus, minus, block_ref, table_ref, sems, target):
    width = plus.shape[0]
    members, depth, _ = target.shape
    half = width // WIDE // 2

    def copy(n):
        return pltpu.make_async_copy(block_ref.at[n % 2], table_ref.at[n], sems.at[n % 2])

    for n in range(half):
        nb = which * half + n
        slot = n % 2
        if n >= 2:
            copy(n - 2).wait()
        for q in range(WIDE // TILE):
            c = lead_ref[0, nb * (WIDE // TILE) + q]
            s = lead_ref[1, nb * (WIDE // TILE) + q]
            c = jnp.broadcast_to(c[None], (width // 16, 16, TILE)).reshape(width, TILE)
            s = jnp.broadcast_to(s[None], (width // 16, 16, TILE)).reshape(width, TILE)
            block_ref[slot, :, q * TILE : (q + 1) * TILE] = (
                c * plus[...] + s * minus[...]
            ).astype(BF16)
        copy(n).start()
        product = jnp.dot(scaled[...], block_ref[slot], preferred_element_type=F32)
        to = slice(n * WIDE, (n + 1) * WIDE)
        target[:, :, to] = product.astype(BF16).reshape(members, depth, WIDE)
    for n in range(half - 2, half):
        copy(n).wait()


def forward_send(
    core_ref, control_ref, row_ref, col_ref, factor_ref, lead_ref, after_ref,
    send_ref, scaled_ref, table_ref,
    control, plus, minus, block_ref, sems, reads,
):
    members, levels, rows, width = control.shape
    copies = [
        pltpu.make_async_copy(control_ref.at[m], control.at[m], reads.at[m]) for m in range(members)
    ]
    for copy in copies:
        copy.start()
    table_factors(factor_ref, width, plus, minus)
    for m in range(members):
        copies[m].wait()
        for l in range(levels):
            amplitude = row_ref[l][:, :1] * col_ref[l : l + 1, :]
            at = (m * levels + l) * rows
            scaled_ref[at : at + rows, :] = (control[m, l] * amplitude).astype(BF16)
    transform(
        1 - core_ref[0], scaled_ref, lead_ref, plus, minus, block_ref, table_ref, sems, send_ref
    )


def forward_own(
    core_ref, scaled_ref, factor_ref, lead_ref, after0_ref, after1_ref,
    own_ref, table_ref, plus, minus, block_ref, sems,
):
    table_factors(factor_ref, plus.shape[0], plus, minus)
    transform(core_ref[0], scaled_ref, lead_ref, plus, minus, block_ref, table_ref, sems, own_ref)


def chip_of(place_ref, h):
    across, along = place_ref[0], place_ref[1]
    return ((across + h // 4) % 2) * 4 + (along + h % 4) % 4


def spread_rows(place_ref, factor_ref, lead_ref, out_ref):
    core = place_ref[2]
    rows = out_ref.shape[1] // 4
    inner_p, inner_m = factor_ref[:rows, :], factor_ref[rows : 2 * rows, :]
    plus, minus = [], []
    for q in range(2):
        slab = chip_of(place_ref, 0) * 2 + (core + q) % 2
        c = jnp.broadcast_to(lead_ref[0, slab][None], (rows // 16, 16, TILE)).reshape(rows, TILE)
        s = jnp.broadcast_to(lead_ref[1, slab][None], (rows // 16, 16, TILE)).reshape(rows, TILE)
        plus.append(c * inner_p + s * inner_m)
        minus.append(c * inner_m - s * inner_p)
    left = lax.broadcasted_iota(jnp.int32, (rows, TILE), 1) < rows
    plus = jnp.where(left, plus[0], plus[1])
    minus = jnp.where(left, minus[0], minus[1])
    nothing = jnp.zeros((rows, TILE), BF16)
    for h in range(out_ref.shape[0]):
        for r in range(2):
            slab = chip_of(place_ref, h) * 2 + (core + r) % 2
            c = factor_ref[pl.ds(2 * rows + slab, 1), :]
            s = factor_ref[pl.ds(2 * rows + 16 + slab, 1), :]
            entry = (c * plus + s * minus).astype(BF16)
            for l in range(2):
                at = slice((2 * l + r) * rows, (2 * l + r + 1) * rows)
                out_ref[h, at, l * TILE : (l + 1) * TILE] = entry
                out_ref[h, at, (1 - l) * TILE : (2 - l) * TILE] = nothing


def pert_of(blocks, at):
    return jnp.concatenate([ref[:, at].reshape(-1, TILE) for ref in blocks], axis=0).astype(F32)


def cells(place_ref, *refs):
    blocks, (own_hbm, par_hbm, rows_ref, cells_hbm, turned_hbm) = refs[:8], refs[8:13]
    own, par, spread, cells_ref, turned_ref, reads, writes = refs[13:]
    members, depth, _ = own.shape
    rows = depth // 2
    last = blocks[0].shape[1] - 1
    loads = [
        pltpu.make_async_copy(own_hbm, own, reads.at[0]),
        pltpu.make_async_copy(par_hbm, par, reads.at[1]),
    ]
    for load in loads:
        load.start()
    lane = lax.broadcasted_iota(jnp.int32, (1, 2 * TILE), 1)
    row = lax.broadcasted_iota(jnp.int32, (4 * rows, 2 * TILE), 0)
    for h, block in enumerate(blocks):
        place = jnp.concatenate(
            [block[r, last].astype(F32)[0:1, :] for r in range(2)], axis=1
        ).astype(jnp.int32)
        level, inside = place // rows, place % rows
        place = level * (2 * rows) + inside + jnp.where(lane < TILE, 0, rows)
        chosen = (row == place).astype(F32).astype(BF16)
        spread[h] = lax.dot_general(
            chosen, rows_ref[h], (((0,), (0,)), ((), ())), preferred_element_type=F32
        ).astype(BF16)
    for load in loads:
        load.wait()
    stores = []
    for k in range(8):
        cols = slice(k * TILE, (k + 1) * TILE)
        along = jnp.concatenate(
            [
                jnp.concatenate(
                    [ref[m, l * rows : (l + 1) * rows, cols] for m in range(members)], axis=1
                )
                for l in range(2)
                for ref in (own, par)
            ],
            axis=0,
        )
        tiles = jnp.concatenate(
            [
                spread[h, r * TILE + k * 16 : r * TILE + (k + 1) * 16, :]
                for h in range(8)
                for r in range(2)
            ],
            axis=0,
        )
        field = jnp.dot(tiles, along, preferred_element_type=F32)
        total = None
        for m in range(members):
            term = pert_of(blocks, k * members + m) * field[:, m * TILE : (m + 1) * TILE]
            total = term if total is None else total + term
        total = total.astype(BF16)
        for h in range(8):
            cells_ref[k, chip_of(place_ref, h)] = total[h * 32 : (h + 1) * 32]
        stores.append(pltpu.make_async_copy(cells_ref.at[k], cells_hbm.at[k], writes.at[k]))
        stores[-1].start()
        turned = jnp.transpose(tiles.astype(F32)).astype(BF16)
        for q in range(2):
            for l in range(2):
                at = (2 * l + q) * rows
                turned_ref[k, (2 * q + l) * rows : (2 * q + l + 1) * rows, :] = turned[at : at + rows]
    stores.append(pltpu.make_async_copy(turned_ref, turned_hbm.at[:8], writes.at[8]))
    stores[-1].start()
    for store in stores:
        store.wait()


def score(cells_ref, own_ref, lent_ref, out_ref):
    copies = out_ref.shape[0]
    total = jnp.sum(cells_ref[...].astype(F32), axis=0)
    value = jnp.concatenate([own_ref[0], lent_ref[0]], axis=0)
    seen = jnp.concatenate([own_ref[1], lent_ref[1]], axis=0)
    resid = total - value
    result = jnp.where(seen > 0.5, resid / jnp.sqrt(1.0 + resid * resid * 0.25), 0.0)
    result = result.astype(BF16)
    for i in range(copies):
        out_ref[i] = result


def back(place_ref, *refs):
    blocks, (score_ref, turned_hbm, own_ref, par_ref, turned, sem) = refs[:8], refs[8:]
    members, depth, _ = own_ref.shape
    load = pltpu.make_async_copy(turned_hbm.at[:8], turned, sem)
    load.start()
    for k in range(8):
        weight = jnp.concatenate(
            [score_ref[k, chip_of(place_ref, h)] for h in range(8)], axis=0
        ).astype(F32)
        weighted = jnp.concatenate(
            [(pert_of(blocks, k * members + m) * weight).astype(BF16) for m in range(members)],
            axis=1,
        )
        if k == 0:
            load.wait()
        result = jnp.dot(turned[k], weighted, preferred_element_type=F32).astype(BF16)
        for m in range(members):
            part = result[:, m * TILE : (m + 1) * TILE]
            own_ref[m, :, k * TILE : (k + 1) * TILE] = part[:depth]
            par_ref[m, :, k * TILE : (k + 1) * TILE] = part[depth:]


def streamed(tables, rows, block_ref, sems):
    steps = tables[0].shape[0]

    def fetch(at):
        return pltpu.make_async_copy(
            tables[at // steps].at[at % steps, rows, :], block_ref.at[at], sems.at[at]
        )

    def block(at):
        if at + 3 < len(tables) * steps:
            fetch(at + 3).start()
        fetch(at).wait()
        return block_ref[at]

    for at in range(3):
        fetch(at).start()
    return block


def inverse_own(core_ref, own_ref, table0_ref, table1_ref, sum_ref, block_ref, sems):
    members, depth, width = own_ref.shape
    core = core_ref[0]
    near = pl.ds(pl.multiple_of(core * width, width), width)
    block = streamed((table0_ref, table1_ref), near, block_ref, sems)
    for n in range(sum_ref.shape[0]):
        sum_ref[n] = jnp.dot(
            own_ref[...].reshape(members * depth, width), block(n), preferred_element_type=F32
        )


def inverse_par(
    core_ref, par_ref, sum_ref, table0_ref, table1_ref, row_ref, col_ref, out_ref,
    piece, sems, block_ref, reads,
):
    members, depth, width = par_ref.shape
    levels, rows, _ = row_ref.shape
    core = core_ref[0]
    steps = sum_ref.shape[0]
    half = steps // 2
    far = pl.ds(pl.multiple_of((1 - core) * width, width), width)
    block = streamed((table0_ref, table1_ref), far, block_ref, reads)

    def copy(n):
        nb = ((1 - core) if n < half else core) * half + n % half
        cols = pl.ds(pl.multiple_of(nb * WIDE, WIDE), WIDE)
        slot = n % piece.shape[0]
        return cols, slot, pltpu.make_async_copy(
            piece.at[slot], out_ref.at[:, :, :, cols], sems.at[slot]
        )

    for n in range(steps):
        cols, slot, store = copy(n)
        product = sum_ref[n] + jnp.dot(
            par_ref[...].reshape(members * depth, width), block(n), preferred_element_type=F32
        )
        product = product.reshape(members, levels, rows, WIDE)
        if n >= piece.shape[0]:
            copy(n - piece.shape[0])[2].wait()
        for l in range(levels):
            amplitude = row_ref[l][:, :1] * col_ref[l : l + 1, cols]
            for m in range(members):
                piece[slot, m, l] = product[m, l] * amplitude
        store.start()
    for n in range(steps - piece.shape[0], steps):
        copy(n)[2].wait()


def shards(control, perturbation, loc_row, loc_col, obs_tile, obs_count, obs_value):
    members, levels, rows, width = control.shape
    slabs = 16
    peers = lax.axis_size("member") * 8
    height = rows * slabs
    half = width // 2
    per_core = half // TILE
    depth = levels * rows
    across = lax.axis_index("across").astype(jnp.int32)
    along = lax.axis_index("along").astype(jnp.int32)
    core = lax.axis_index("core").astype(jnp.int32)
    group = lax.axis_index("member").astype(jnp.int32)
    core_index = core.reshape(1)
    place = jnp.stack([across, along, core])
    swap = [(0, 1), (1, 0)]

    def from_next(array, step):
        return lax.ppermute(array, "along", [((i + step) % 4, i) for i in range(4)])

    blocks = per_core * members + 1
    own_tiles, send_tiles = run(
        select,
        [bf16(blocks, 16, TILE)] * 2,
        [SMEM, HBM, HBM],
        1 << 27,
        [
            pltpu.VMEM((2, TILE), jnp.int32),
            pltpu.VMEM(perturbation.shape, BF16),
            pltpu.SemaphoreType.DMA((members + 1,)),
        ],
    )(core_index, obs_tile.reshape(2, TILE), perturbation)
    here = jnp.stack([own_tiles, lax.ppermute(send_tiles, "core", swap)])
    facing = lax.ppermute(here, "across", swap)
    here2 = from_next(here, 2)
    here1, here3 = from_next(here, 1), from_next(here, 3)
    facing1, facing3 = from_next(facing, 1), from_next(facing, 3)
    facing2 = lax.ppermute(here2, "across", swap)
    arrived = (here, here1, here2, here3, facing, facing1, facing2, facing3)

    lane = jnp.arange(TILE, dtype=jnp.int32)

    def of_column(column, array):
        return lax.dynamic_slice_in_dim(array, column * 16, 16, 0)

    seen = (lane[None, :] < obs_count[:, None]).astype(F32)
    mine = per_core * core + group
    other = per_core * (1 - core) + group
    stated = jnp.stack([of_column(mine, obs_value), of_column(mine, seen)])
    lent = jnp.stack([of_column(other, obs_value), of_column(other, seen)])
    lent = lax.ppermute(lent, "core", swap)

    lead = cas(np.arange(16), np.arange(16), 16)
    lead = jnp.asarray(np.repeat(np.stack(lead[2:])[:, :, :, None], TILE, axis=3))
    inner = 64
    outer = cas(np.arange(width // inner), np.arange(TILE), width // inner)
    near = cas(np.arange(inner), np.arange(TILE), width)
    root = np.float32(np.sqrt(width))
    factors = jnp.asarray(np.concatenate([outer[2], outer[3], near[0] / root, near[1] / root]))
    wave = np.arange(TILE) % rows
    base = cas(np.arange(rows), wave, height)
    turn = cas(np.arange(16), wave, 16)
    root = np.float32(np.sqrt(height))
    row_factors = jnp.asarray(np.concatenate([base[0] / root, base[1] / root, turn[2], turn[3]]))

    row_b = jnp.broadcast_to(loc_row[:, :, None], (levels, rows, TILE))
    table_half = bf16(width // WIDE // 2, width, WIDE)
    work = [
        pltpu.VMEM((width, TILE), F32),
        pltpu.VMEM((width, TILE), F32),
        pltpu.VMEM((2, width, WIDE), BF16),
        pltpu.SemaphoreType.DMA((2,)),
    ]
    flops = members * depth * width * width
    send, scaled, table0 = run(
        forward_send,
        [bf16(members, depth, half), bf16(members * depth, width), table_half],
        [SMEM, HBM, VMEM, VMEM, VMEM, VMEM, HBM],
        flops,
        [pltpu.VMEM(control.shape, F32)] + work + [pltpu.SemaphoreType.DMA((members,))],
        [VMEM, VMEM, HBM],
        mib=48,
    )(core_index, control, row_b, loc_col, factors, lead, here)
    par = lax.ppermute(send, "core", swap)
    own, table1 = run(
        forward_own,
        [bf16(members, depth, half), table_half],
        [SMEM, VMEM, VMEM, VMEM, HBM, HBM],
        flops,
        work,
        [VMEM, HBM],
        mib=48,
    )(core_index, scaled, factors, lead, facing, here2)
    table_rows = run(
        spread_rows, bf16(8, 4 * rows, 2 * TILE), [SMEM, VMEM, VMEM], 1 << 22
    )(place, row_factors, lead)

    tiles = slabs * 16
    partial, turned = run(
        cells,
        [bf16(per_core, 8, 2 * 16, TILE), bf16(12 * per_core, 4 * rows, tiles)],
        [SMEM] + [VMEM] * 8 + [HBM, HBM, VMEM],
        1 << 30,
        [
            pltpu.VMEM((members, depth, half), BF16),
            pltpu.VMEM((members, depth, half), BF16),
            pltpu.VMEM((8, tiles, 4 * rows), BF16),
            pltpu.VMEM((per_core, 8, 2 * 16, TILE), BF16),
            pltpu.VMEM((per_core, 4 * rows, tiles), BF16),
            pltpu.SemaphoreType.DMA((2,)),
            pltpu.SemaphoreType.DMA((9,)),
        ],
        [HBM, HBM],
    )(place, *arrived, own, par, table_rows)
    partial = lax.all_to_all(
        partial.reshape(peers, 2 * 16, TILE), SAME_CORE, split_axis=0, concat_axis=0, tiled=True
    )
    scores = run(score, bf16(peers, 2 * 16, TILE), [VMEM] * 3, 1 << 20)(partial, stated, lent)
    scores = lax.all_to_all(scores, SAME_CORE, split_axis=0, concat_axis=0, tiled=True)

    back_own, back_send = run(
        back,
        [bf16(members, depth, half)] * 2,
        [SMEM] + [VMEM] * 9 + [HBM],
        1 << 28,
        [pltpu.VMEM((per_core, 4 * rows, tiles), BF16), pltpu.SemaphoreType.DMA],
        mib=46,
    )(place, *arrived, scores.reshape(per_core, 8, 2 * 16, TILE), turned)
    back_other = lax.ppermute(back_send, "core", swap)
    parts = width // WIDE
    stream = [pltpu.VMEM((parts, half, WIDE), BF16), pltpu.SemaphoreType.DMA((parts,))]
    summed = run(
        inverse_own,
        f32(width // WIDE, members * depth, WIDE),
        [SMEM, VMEM, HBM, HBM],
        flops,
        stream,
        mib=46,
    )(core_index, back_own, table0, table1)
    return run(
        inverse_par,
        f32(*control.shape),
        [SMEM, VMEM, VMEM, HBM, HBM, VMEM, VMEM],
        flops,
        [pltpu.VMEM((2, members, levels, rows, WIDE), F32), pltpu.SemaphoreType.DMA((2,))] + stream,
        [HBM],
        mib=46,
    )(core_index, back_other, summed, table0, table1, row_b, loc_col)


def solution(mesh):
    torus = Mesh(
        mesh.devices.reshape(mesh.shape["member"], 2, 4, 2),
        ("member", "across", "along", "core"),
    )
    placed = (
        P("member", None, SLAB, None),
        P("member", None, SLAB, None),
        P(None, SLAB),
        P(),
        P(SLAB),
        P(SLAB),
        P(SLAB, None),
    )
    return jax.shard_map(
        shards,
        mesh=torus,
        in_specs=placed,
        out_specs=P("member", None, SLAB, None),
        check_vma=False,
    )
```

```python
import jax
import jax.numpy as jnp
import numpy as np
from jax import lax
from jax.experimental import pallas as pl
from jax.experimental.pallas import tpu as pltpu
from jax.sharding import Mesh
from jax.sharding import PartitionSpec as P

TILE = 128
WIDE = 256
LEAD = 192
BF16 = jnp.bfloat16
F32 = jnp.float32
SLAB = ("across", "along", "core")
SAME_CORE = ("member", "across", "along")
VMEM = pl.BlockSpec(memory_space=pltpu.VMEM)
SMEM = pl.BlockSpec(memory_space=pltpu.SMEM)
HBM = pl.BlockSpec(memory_space=pltpu.HBM)


def run(kernel, out_shape, in_specs, flops, scratch=(), out_specs=None, mib=46):
    outs = out_shape if isinstance(out_shape, list) else [out_shape]
    if out_specs is None:
        out_specs = [VMEM] * len(outs)
    moved = sum(int(np.prod(o.shape)) * o.dtype.itemsize for o in outs) * 2
    call = pl.pallas_call(
        kernel,
        in_specs=in_specs,
        out_specs=out_specs,
        out_shape=outs,
        scratch_shapes=list(scratch),
        compiler_params=pltpu.CompilerParams(vmem_limit_bytes=mib << 20),
        cost_estimate=pl.CostEstimate(flops=flops, bytes_accessed=moved, transcendentals=0),
    )

    def launch(*args):
        results = call(*args)
        return results if isinstance(out_shape, list) else results[0]

    return launch


def bf16(*shape):
    return jax.ShapeDtypeStruct(shape, BF16)


def f32(*shape):
    return jax.ShapeDtypeStruct(shape, F32)


def cas(first, second, order):
    angle = 2.0 * np.pi * (np.outer(first, second) % order) / order
    c, s = np.cos(angle), np.sin(angle)
    return [a.astype(np.float32) for a in (c + s, c - s, c, s)]


def select(core_ref, tile_ref, pert_ref, own_ref, send_ref, tiles, pert, sems):
    members = pert.shape[0]
    core = core_ref[0]
    copies = [pltpu.make_async_copy(tile_ref, tiles, sems.at[members])]
    copies += [pltpu.make_async_copy(pert_ref.at[m], pert.at[m], sems.at[m]) for m in range(members)]
    for copy in copies:
        copy.start()
    copies[0].wait()
    place = tiles[...] // 16
    row = lax.broadcasted_iota(jnp.int32, (TILE, TILE), 0)
    halves = []
    for half in (1 - core, core):
        mine = jnp.where(half == 0, place[0:1, :], place[1:2, :])
        halves.append((mine, jnp.transpose((row == mine).astype(F32)).astype(BF16)))
    for copy in copies[1:]:
        copy.wait()
    for ref, half, (mine, chosen) in zip((send_ref, own_ref), (1 - core, core), halves):
        for k in range(8):
            cols = pl.ds(pl.multiple_of((half * 8 + k) * TILE, TILE), TILE)
            tile = jnp.concatenate(
                [pert[m, :, :, cols].reshape(TILE, TILE) for m in range(members)], axis=1
            )
            rows = jnp.dot(
                chosen[16 * k : 16 * k + 16], tile, preferred_element_type=F32
            ).astype(BF16)
            for m in range(members):
                ref[k * members + m] = rows[:, m * TILE : (m + 1) * TILE]
        ref[8 * members] = jnp.broadcast_to(mine.astype(F32), (16, TILE)).astype(BF16)


def lead_of(factor_ref, part, index):
    at = pl.multiple_of(LEAD + part * 256 + index * 16, 16)
    return factor_ref[pl.ds(at, 16), :]


def table_factors(factor_ref, width, plus, minus):
    inner = 64
    outer = width // inner
    near_p = factor_ref[2 * outer : 2 * outer + inner, :]
    near_m = factor_ref[2 * outer + inner : 2 * outer + 2 * inner, :]
    for u in range(outer):
        at = slice(u * inner, (u + 1) * inner)
        c, s = factor_ref[u : u + 1, :], factor_ref[outer + u : outer + u + 1, :]
        plus[at, :] = c * near_p + s * near_m
        minus[at, :] = c * near_m - s * near_p


def transform(which, scaled, factor_ref, plus, minus, block_ref, table_ref, sems, target):
    width = plus.shape[0]
    members, depth, _ = target.shape
    half = width // WIDE // 2

    def copy(nb, slot):
        return pltpu.make_async_copy(block_ref.at[slot], table_ref.at[nb], sems.at[slot])

    def step(n, carry):
        nb = which * half + n
        slot = lax.rem(n, 2)

        @pl.when(n >= 2)
        def _():
            copy(n - 2, slot).wait()

        for q in range(WIDE // TILE):
            c = lead_of(factor_ref, 0, nb * (WIDE // TILE) + q)
            s = lead_of(factor_ref, 1, nb * (WIDE // TILE) + q)
            c = jnp.broadcast_to(c[None], (width // 16, 16, TILE)).reshape(width, TILE)
            s = jnp.broadcast_to(s[None], (width // 16, 16, TILE)).reshape(width, TILE)
            block_ref[slot, :, q * TILE : (q + 1) * TILE] = (
                c * plus[...] + s * minus[...]
            ).astype(BF16)
        copy(n, slot).start()
        product = jnp.dot(scaled[...], block_ref[slot], preferred_element_type=F32)
        to = pl.ds(pl.multiple_of(n * WIDE, WIDE), WIDE)
        target[:, :, to] = product.astype(BF16).reshape(members, depth, WIDE)
        return carry

    lax.fori_loop(0, half, step, 0)
    for slot in range(2):
        copy(slot, slot).wait()


def forward_send(
    core_ref, control_ref, row_ref, col_ref, factor_ref, after_ref,
    send_ref, scaled_hbm, table_ref,
    control, scaled_ref, plus, minus, block_ref, sems, reads, kept,
):
    members, levels, rows, width = control.shape
    copies = [
        pltpu.make_async_copy(control_ref.at[m], control.at[m], reads.at[m]) for m in range(members)
    ]
    for copy in copies:
        copy.start()
    table_factors(factor_ref, width, plus, minus)
    for m in range(members):
        copies[m].wait()
        for l in range(levels):
            amplitude = row_ref[l][:, :1] * col_ref[l : l + 1, :]
            at = (m * levels + l) * rows
            scaled_ref[at : at + rows, :] = (control[m, l] * amplitude).astype(BF16)
    keep = pltpu.make_async_copy(scaled_ref, scaled_hbm.at[: scaled_ref.shape[0]], kept)
    keep.start()
    transform(
        1 - core_ref[0], scaled_ref, factor_ref, plus, minus, block_ref, table_ref, sems, send_ref
    )
    keep.wait()


def forward_own(
    core_ref, scaled_hbm, factor_ref, after0_ref, after1_ref,
    own_ref, table_ref, scaled_ref, plus, minus, block_ref, sems, kept,
):
    load = pltpu.make_async_copy(scaled_hbm.at[: scaled_ref.shape[0]], scaled_ref, kept)
    load.start()
    table_factors(factor_ref, plus.shape[0], plus, minus)
    load.wait()
    transform(core_ref[0], scaled_ref, factor_ref, plus, minus, block_ref, table_ref, sems, own_ref)


def chip_of(place_ref, h):
    across, along = place_ref[0] // 8, place_ref[0] // 2 % 4
    return ((across + h // 4) % 2) * 4 + (along + h % 4) % 4


def spread_rows(place_ref, factor_ref, out_ref):
    core = place_ref[0] % 2
    rows = out_ref.shape[1] // 4
    first = factor_ref.shape[0] - 2 * rows - 32
    inner_p = factor_ref[first : first + rows, :]
    inner_m = factor_ref[first + rows : first + 2 * rows, :]
    plus, minus = [], []
    for q in range(2):
        slab = chip_of(place_ref, 0) * 2 + (core + q) % 2
        c = jnp.broadcast_to(lead_of(factor_ref, 0, slab)[None], (rows // 16, 16, TILE)).reshape(rows, TILE)
        s = jnp.broadcast_to(lead_of(factor_ref, 1, slab)[None], (rows // 16, 16, TILE)).reshape(rows, TILE)
        plus.append(c * inner_p + s * inner_m)
        minus.append(c * inner_m - s * inner_p)
    left = lax.broadcasted_iota(jnp.int32, (rows, TILE), 1) < rows
    plus = jnp.where(left, plus[0], plus[1])
    minus = jnp.where(left, minus[0], minus[1])
    nothing = jnp.zeros((rows, TILE), BF16)
    for h in range(out_ref.shape[0]):
        for r in range(2):
            slab = chip_of(place_ref, h) * 2 + (core + r) % 2
            c = factor_ref[pl.ds(first + 2 * rows + slab, 1), :]
            s = factor_ref[pl.ds(first + 2 * rows + 16 + slab, 1), :]
            entry = (c * plus + s * minus).astype(BF16)
            for l in range(2):
                at = slice((2 * l + r) * rows, (2 * l + r + 1) * rows)
                out_ref[h, at, l * TILE : (l + 1) * TILE] = entry
                out_ref[h, at, (1 - l) * TILE : (2 - l) * TILE] = nothing


def pert_of(blocks, at):
    return jnp.concatenate([ref[:, at].reshape(-1, TILE) for ref in blocks], axis=0).astype(F32)


def cells(place_ref, *refs):
    blocks, (own_hbm, par_hbm, rows_ref, cells_hbm, turned_hbm) = refs[:8], refs[8:13]
    own, par, spread, cells_ref, turned_ref, reads, writes = refs[13:]
    members, depth, _ = own.shape
    rows = depth // 2
    last = blocks[0].shape[1] - 1
    loads = [
        pltpu.make_async_copy(own_hbm, own, reads.at[0]),
        pltpu.make_async_copy(par_hbm, par, reads.at[1]),
    ]
    for load in loads:
        load.start()
    lane = lax.broadcasted_iota(jnp.int32, (1, 2 * TILE), 1)
    row = lax.broadcasted_iota(jnp.int32, (4 * rows, 2 * TILE), 0)
    for h, block in enumerate(blocks):
        place = jnp.concatenate(
            [block[r, last].astype(F32)[0:1, :] for r in range(2)], axis=1
        ).astype(jnp.int32)
        level, inside = place // rows, place % rows
        place = level * (2 * rows) + inside + jnp.where(lane < TILE, 0, rows)
        chosen = (row == place).astype(F32).astype(BF16)
        spread[h] = lax.dot_general(
            chosen, rows_ref[h], (((0,), (0,)), ((), ())), preferred_element_type=F32
        ).astype(BF16)
    for load in loads:
        load.wait()
    stores = []
    for k in range(8):
        cols = slice(k * TILE, (k + 1) * TILE)
        along = jnp.concatenate(
            [
                jnp.concatenate(
                    [ref[m, l * rows : (l + 1) * rows, cols] for m in range(members)], axis=1
                )
                for l in range(2)
                for ref in (own, par)
            ],
            axis=0,
        )
        tiles = jnp.concatenate(
            [
                spread[h, r * TILE + k * 16 : r * TILE + (k + 1) * 16, :]
                for h in range(8)
                for r in range(2)
            ],
            axis=0,
        )
        field = jnp.dot(tiles, along, preferred_element_type=F32)
        total = None
        for m in range(members):
            term = pert_of(blocks, k * members + m) * field[:, m * TILE : (m + 1) * TILE]
            total = term if total is None else total + term
        total = total.astype(BF16)
        for h in range(8):
            cells_ref[k, chip_of(place_ref, h)] = total[h * 32 : (h + 1) * 32]
        stores.append(pltpu.make_async_copy(cells_ref.at[k], cells_hbm.at[k], writes.at[k]))
        stores[-1].start()
        turned = jnp.transpose(tiles.astype(F32)).astype(BF16)
        for q in range(2):
            for l in range(2):
                at = (2 * l + q) * rows
                turned_ref[k, (2 * q + l) * rows : (2 * q + l + 1) * rows, :] = turned[at : at + rows]
    stores.append(pltpu.make_async_copy(turned_ref, turned_hbm.at[:8], writes.at[8]))
    stores[-1].start()
    for store in stores:
        store.wait()


def score(cells_ref, own_ref, lent_ref, out_ref):
    copies = out_ref.shape[0]
    total = jnp.sum(cells_ref[...].astype(F32), axis=0)
    value = jnp.concatenate([own_ref[0], lent_ref[0]], axis=0)
    seen = jnp.concatenate([own_ref[1], lent_ref[1]], axis=0)
    resid = total - value
    result = jnp.where(seen > 0.5, resid / jnp.sqrt(1.0 + resid * resid * 0.25), 0.0)
    result = result.astype(BF16)
    for i in range(copies):
        out_ref[i] = result


def back(place_ref, *refs):
    blocks, (score_ref, turned_hbm, own_ref, par_ref, turned, sem) = refs[:8], refs[8:]
    members, depth, _ = own_ref.shape
    load = pltpu.make_async_copy(turned_hbm.at[:8], turned, sem)
    load.start()
    for k in range(8):
        weight = jnp.concatenate(
            [score_ref[k, chip_of(place_ref, h)] for h in range(8)], axis=0
        ).astype(F32)
        weighted = jnp.concatenate(
            [(pert_of(blocks, k * members + m) * weight).astype(BF16) for m in range(members)],
            axis=1,
        )
        if k == 0:
            load.wait()
        result = jnp.dot(turned[k], weighted, preferred_element_type=F32).astype(BF16)
        for m in range(members):
            part = result[:, m * TILE : (m + 1) * TILE]
            own_ref[m, :, k * TILE : (k + 1) * TILE] = part[:depth]
            par_ref[m, :, k * TILE : (k + 1) * TILE] = part[depth:]


def streamed(tables, rows, block_ref, sems):
    steps = tables[0].shape[0]

    def fetch(i, n):
        at = i * steps + n
        return pltpu.make_async_copy(tables[i].at[n, rows, :], block_ref.at[at], sems.at[at])

    for n in range(3):
        fetch(0, n).start()

    def block(i, n):
        @pl.when(n + 3 < steps)
        def _():
            fetch(i, n + 3).start()

        if i + 1 < len(tables):

            @pl.when(n + 3 >= steps)
            def _():
                fetch(i + 1, n + 3 - steps).start()

        fetch(i, n).wait()
        return block_ref[i * steps + n]

    return block


def inverse_own(core_ref, own_ref, table0_ref, table1_ref, sum_ref, block_ref, sems):
    members, depth, width = own_ref.shape
    near = pl.ds(pl.multiple_of(core_ref[0] * width, width), width)
    half = table0_ref.shape[0]
    core = core_ref[0]
    block = streamed((table0_ref, table1_ref), near, block_ref, sems)
    for i in range(2):
        which = (1 - core) if i == 0 else core

        def step(n, carry, i=i, which=which):
            sum_ref[which * half + n] = jnp.dot(
                own_ref[...].reshape(members * depth, width),
                block(i, n),
                preferred_element_type=F32,
            )
            return carry

        lax.fori_loop(0, half, step, 0)


def inverse_par(
    core_ref, par_ref, sum_ref, table0_ref, table1_ref, row_ref, col_ref, out_ref,
    piece, sems, block_ref, reads,
):
    members, depth, width = par_ref.shape
    levels, rows, _ = row_ref.shape
    core = core_ref[0]
    half = table0_ref.shape[0]
    far = pl.ds(pl.multiple_of((1 - core) * width, width), width)

    def copy(nb, slot):
        cols = pl.ds(pl.multiple_of(nb * WIDE, WIDE), WIDE)
        return pltpu.make_async_copy(piece.at[slot], out_ref.at[:, :, :, cols], sems.at[slot])

    block = streamed((table0_ref, table1_ref), far, block_ref, reads)
    for i in range(2):
        which = (1 - core) if i == 0 else core

        def step(n, carry, i=i, which=which):
            slot = lax.rem(n, 2)
            nb = which * half + n
            cols = pl.ds(pl.multiple_of(nb * WIDE, WIDE), WIDE)
            product = sum_ref[nb] + jnp.dot(
                par_ref[...].reshape(members * depth, width),
                block(i, n),
                preferred_element_type=F32,
            )
            product = product.reshape(members, levels, rows, WIDE)

            @pl.when(n >= (2 if i == 0 else 0))
            def _():
                copy(nb, slot).wait()

            for l in range(levels):
                amplitude = row_ref[l][:, :1] * col_ref[l : l + 1, cols]
                for m in range(members):
                    piece[slot, m, l] = product[m, l] * amplitude
            copy(nb, slot).start()
            return carry

        lax.fori_loop(0, half, step, 0)
    for slot in range(2):
        copy(slot, slot).wait()


def shards(control, perturbation, loc_row, loc_col, obs_tile, obs_count, obs_value):
    members, levels, rows, width = control.shape
    slabs = 16
    peers = lax.axis_size("member") * 8
    height = rows * slabs
    half = width // 2
    per_core = half // TILE
    depth = levels * rows
    across = lax.axis_index("across").astype(jnp.int32)
    along = lax.axis_index("along").astype(jnp.int32)
    core = lax.axis_index("core").astype(jnp.int32)
    group = lax.axis_index("member").astype(jnp.int32)
    core_index = core.reshape(1)
    place = (across * 8 + along * 2 + core).reshape(1)
    swap = [(0, 1), (1, 0)]

    def from_next(array, step):
        return lax.ppermute(array, "along", [((i + step) % 4, i) for i in range(4)])

    blocks = per_core * members + 1
    own_tiles, send_tiles = run(
        select,
        [bf16(blocks, 16, TILE)] * 2,
        [SMEM, HBM, HBM],
        1 << 27,
        [
            pltpu.VMEM((2, TILE), jnp.int32),
            pltpu.VMEM(perturbation.shape, BF16),
            pltpu.SemaphoreType.DMA((members + 1,)),
        ],
    )(core_index, obs_tile.reshape(2, TILE), perturbation)
    here = jnp.stack([own_tiles, lax.ppermute(send_tiles, "core", swap)])
    facing = lax.ppermute(here, "across", swap)
    here2 = from_next(here, 2)
    here1, here3 = from_next(here, 1), from_next(here, 3)
    facing1, facing3 = from_next(facing, 1), from_next(facing, 3)
    facing2 = lax.ppermute(here2, "across", swap)
    arrived = (here, here1, here2, here3, facing, facing1, facing2, facing3)

    lane = jnp.arange(TILE, dtype=jnp.int32)

    def of_column(column, array):
        return lax.dynamic_slice_in_dim(array, column * 16, 16, 0)

    seen = (lane[None, :] < obs_count[:, None]).astype(F32)
    mine = per_core * core + group
    other = per_core * (1 - core) + group
    stated = jnp.stack([of_column(mine, obs_value), of_column(mine, seen)])
    lent = jnp.stack([of_column(other, obs_value), of_column(other, seen)])
    lent = lax.ppermute(lent, "core", swap)

    lead = cas(np.arange(16), np.arange(16), 16)
    lead = np.repeat(np.stack(lead[2:]).reshape(-1, 1), TILE, axis=1)
    inner = 64
    outer = cas(np.arange(width // inner), np.arange(TILE), width // inner)
    near = cas(np.arange(inner), np.arange(TILE), width)
    root = np.float32(np.sqrt(width))
    factors = [outer[2], outer[3], near[0] / root, near[1] / root, lead]
    wave = np.arange(TILE) % rows
    base = cas(np.arange(rows), wave, height)
    turn = cas(np.arange(16), wave, 16)
    root = np.float32(np.sqrt(height))
    factors += [base[0] / root, base[1] / root, turn[2], turn[3]]
    factors = jnp.asarray(np.concatenate(factors))

    row_b = jnp.broadcast_to(loc_row[:, :, None], (levels, rows, TILE))
    table_half = bf16(width // WIDE // 2, width, WIDE)
    work = [
        pltpu.VMEM((members * depth, width), BF16),
        pltpu.VMEM((width, TILE), F32),
        pltpu.VMEM((width, TILE), F32),
        pltpu.VMEM((2, width, WIDE), BF16),
        pltpu.SemaphoreType.DMA((2,)),
    ]
    flops = members * depth * width * width
    send, scaled, table0 = run(
        forward_send,
        [bf16(members, depth, half), bf16(6 * members * depth, width), table_half],
        [SMEM, HBM, VMEM, VMEM, VMEM, HBM],
        flops,
        [pltpu.VMEM(control.shape, F32)]
        + work
        + [pltpu.SemaphoreType.DMA((members,)), pltpu.SemaphoreType.DMA],
        [VMEM, HBM, HBM],
        mib=50,
    )(core_index, control, row_b, loc_col, factors, here)
    par = lax.ppermute(send, "core", swap)
    own, table1 = run(
        forward_own,
        [bf16(members, depth, half), table_half],
        [SMEM, HBM, VMEM, HBM, HBM],
        flops,
        work + [pltpu.SemaphoreType.DMA],
        [VMEM, HBM],
        mib=50,
    )(core_index, scaled, factors, facing, here2)
    table_rows = run(
        spread_rows, bf16(8, 4 * rows, 2 * TILE), [SMEM, VMEM], 1 << 22
    )(place, factors)

    tiles = slabs * 16
    partial, turned = run(
        cells,
        [bf16(per_core, 8, 2 * 16, TILE), bf16(12 * per_core, 4 * rows, tiles)],
        [SMEM] + [VMEM] * 8 + [HBM, HBM, VMEM],
        1 << 30,
        [
            pltpu.VMEM((members, depth, half), BF16),
            pltpu.VMEM((members, depth, half), BF16),
            pltpu.VMEM((8, tiles, 4 * rows), BF16),
            pltpu.VMEM((per_core, 8, 2 * 16, TILE), BF16),
            pltpu.VMEM((per_core, 4 * rows, tiles), BF16),
            pltpu.SemaphoreType.DMA((2,)),
            pltpu.SemaphoreType.DMA((9,)),
        ],
        [HBM, HBM],
    )(place, *arrived, own, par, table_rows)
    partial = lax.all_to_all(
        partial.reshape(peers, 2 * 16, TILE), SAME_CORE, split_axis=0, concat_axis=0, tiled=True
    )
    scores = run(score, bf16(peers, 2 * 16, TILE), [VMEM] * 3, 1 << 20)(partial, stated, lent)
    scores = lax.all_to_all(scores, SAME_CORE, split_axis=0, concat_axis=0, tiled=True)

    back_own, back_send = run(
        back,
        [bf16(members, depth, half)] * 2,
        [SMEM] + [VMEM] * 9 + [HBM],
        1 << 28,
        [pltpu.VMEM((per_core, 4 * rows, tiles), BF16), pltpu.SemaphoreType.DMA],
        mib=46,
    )(place, *arrived, scores.reshape(per_core, 8, 2 * 16, TILE), turned)
    back_other = lax.ppermute(back_send, "core", swap)
    parts = width // WIDE
    stream = [pltpu.VMEM((parts, half, WIDE), BF16), pltpu.SemaphoreType.DMA((parts,))]
    summed = run(
        inverse_own,
        f32(width // WIDE, members * depth, WIDE),
        [SMEM, VMEM, HBM, HBM],
        flops,
        stream,
        mib=46,
    )(core_index, back_own, table0, table1)
    return run(
        inverse_par,
        f32(*control.shape),
        [SMEM, VMEM, VMEM, HBM, HBM, VMEM, VMEM],
        flops,
        [pltpu.VMEM((2, members, levels, rows, WIDE), F32), pltpu.SemaphoreType.DMA((2,))] + stream,
        [HBM],
        mib=46,
    )(core_index, back_other, summed, table0, table1, row_b, loc_col)


def solution(mesh):
    torus = Mesh(
        mesh.devices.reshape(mesh.shape["member"], 2, 4, 2),
        ("member", "across", "along", "core"),
    )
    placed = (
        P("member", None, SLAB, None),
        P("member", None, SLAB, None),
        P(None, SLAB),
        P(),
        P(SLAB),
        P(SLAB),
        P(SLAB, None),
    )
    return jax.shard_map(
        shards,
        mesh=torus,
        in_specs=placed,
        out_specs=P("member", None, SLAB, None),
        check_vma=False,
    )
```

```python
import jax
import jax.numpy as jnp
import numpy as np
from jax import lax
from jax.experimental import pallas as pl
from jax.experimental.pallas import tpu as pltpu
from jax.sharding import Mesh
from jax.sharding import PartitionSpec as P

TILE = 128
WIDE = 256
LEAD = 192
BF16 = jnp.bfloat16
F32 = jnp.float32
SLAB = ("across", "along", "core")
SAME_CORE = ("member", "across", "along")
VMEM = pl.BlockSpec(memory_space=pltpu.VMEM)
SMEM = pl.BlockSpec(memory_space=pltpu.SMEM)
HBM = pl.BlockSpec(memory_space=pltpu.HBM)


def run(kernel, out_shape, in_specs, flops, scratch=(), out_specs=None, mib=46):
    outs = out_shape if isinstance(out_shape, list) else [out_shape]
    if out_specs is None:
        out_specs = [VMEM] * len(outs)
    moved = sum(int(np.prod(o.shape)) * o.dtype.itemsize for o in outs) * 2
    call = pl.pallas_call(
        kernel,
        in_specs=in_specs,
        out_specs=out_specs,
        out_shape=outs,
        scratch_shapes=list(scratch),
        compiler_params=pltpu.CompilerParams(vmem_limit_bytes=mib << 20),
        cost_estimate=pl.CostEstimate(flops=flops, bytes_accessed=moved, transcendentals=0),
    )

    def launch(*args):
        results = call(*args)
        return results if isinstance(out_shape, list) else results[0]

    return launch


def bf16(*shape):
    return jax.ShapeDtypeStruct(shape, BF16)


def f32(*shape):
    return jax.ShapeDtypeStruct(shape, F32)


def cas(first, second, order):
    angle = 2.0 * np.pi * (np.outer(first, second) % order) / order
    c, s = np.cos(angle), np.sin(angle)
    return [a.astype(np.float32) for a in (c + s, c - s, c, s)]


def select(core_ref, tile_ref, pert_ref, own_ref, send_ref, tiles, pert, sems):
    members = pert.shape[0]
    core = core_ref[0]
    copies = [pltpu.make_async_copy(tile_ref, tiles, sems.at[members])]
    copies += [pltpu.make_async_copy(pert_ref.at[m], pert.at[m], sems.at[m]) for m in range(members)]
    for copy in copies:
        copy.start()
    copies[0].wait()
    place = tiles[...] // 16
    row = lax.broadcasted_iota(jnp.int32, (TILE, TILE), 0)
    halves = []
    for half in (1 - core, core):
        mine = jnp.where(half == 0, place[0:1, :], place[1:2, :])
        halves.append((mine, jnp.transpose((row == mine).astype(F32)).astype(BF16)))
    for copy in copies[1:]:
        copy.wait()
    for ref, half, (mine, chosen) in zip((send_ref, own_ref), (1 - core, core), halves):
        for k in range(8):
            cols = pl.ds(pl.multiple_of((half * 8 + k) * TILE, TILE), TILE)
            tile = jnp.concatenate(
                [pert[m, :, :, cols].reshape(TILE, TILE) for m in range(members)], axis=1
            )
            rows = jnp.dot(
                chosen[16 * k : 16 * k + 16], tile, preferred_element_type=F32
            ).astype(BF16)
            for m in range(members):
                ref[k * members + m] = rows[:, m * TILE : (m + 1) * TILE]
        ref[8 * members] = jnp.broadcast_to(mine.astype(F32), (16, TILE)).astype(BF16)


def lead_of(factor_ref, part, index):
    at = pl.multiple_of(LEAD + part * 256 + index * 16, 16)
    return factor_ref[pl.ds(at, 16), :]


def table_factors(factor_ref, width, plus, minus):
    inner = 64
    outer = width // inner
    near_p = factor_ref[2 * outer : 2 * outer + inner, :]
    near_m = factor_ref[2 * outer + inner : 2 * outer + 2 * inner, :]
    for u in range(outer):
        at = slice(u * inner, (u + 1) * inner)
        c, s = factor_ref[u : u + 1, :], factor_ref[outer + u : outer + u + 1, :]
        plus[at, :] = c * near_p + s * near_m
        minus[at, :] = c * near_m - s * near_p


def transform(which, scaled, factor_ref, plus, minus, block_ref, table_ref, sems, target):
    width = plus.shape[0]
    members, depth, _ = target.shape
    half = width // WIDE // 2

    def copy(nb, slot):
        return pltpu.make_async_copy(block_ref.at[slot], table_ref.at[nb], sems.at[slot])

    def step(n, carry):
        nb = which * half + n
        slot = lax.rem(n, 2)

        @pl.when(n >= 2)
        def _():
            copy(n - 2, slot).wait()

        for q in range(WIDE // TILE):
            c = lead_of(factor_ref, 0, nb * (WIDE // TILE) + q)
            s = lead_of(factor_ref, 1, nb * (WIDE // TILE) + q)
            c = jnp.broadcast_to(c[None], (width // 16, 16, TILE)).reshape(width, TILE)
            s = jnp.broadcast_to(s[None], (width // 16, 16, TILE)).reshape(width, TILE)
            block_ref[slot, :, q * TILE : (q + 1) * TILE] = (
                c * plus[...] + s * minus[...]
            ).astype(BF16)
        copy(n, slot).start()
        product = jnp.dot(scaled[...], block_ref[slot], preferred_element_type=F32)
        to = pl.ds(pl.multiple_of(n * WIDE, WIDE), WIDE)
        target[:, :, to] = product.astype(BF16).reshape(members, depth, WIDE)
        return carry

    lax.fori_loop(0, half, step, 0)
    for slot in range(2):
        copy(slot, slot).wait()


def forward_send(
    core_ref, control_ref, row_ref, col_ref, factor_ref, after_ref,
    send_ref, scaled_hbm, table_ref,
    control, scaled_ref, plus, minus, block_ref, sems, reads, kept,
):
    members, levels, rows, width = control.shape
    copies = [
        pltpu.make_async_copy(control_ref.at[m], control.at[m], reads.at[m]) for m in range(members)
    ]
    for copy in copies:
        copy.start()
    table_factors(factor_ref, width, plus, minus)
    for m in range(members):
        copies[m].wait()
        for l in range(levels):
            amplitude = row_ref[l][:, :1] * col_ref[l : l + 1, :]
            at = (m * levels + l) * rows
            scaled_ref[at : at + rows, :] = (control[m, l] * amplitude).astype(BF16)
    keep = pltpu.make_async_copy(scaled_ref, scaled_hbm.at[: scaled_ref.shape[0]], kept)
    keep.start()
    transform(
        1 - core_ref[0], scaled_ref, factor_ref, plus, minus, block_ref, table_ref, sems, send_ref
    )
    keep.wait()


def forward_own(
    core_ref, scaled_hbm, factor_ref, after0_ref, after1_ref,
    own_ref, table_ref, scaled_ref, plus, minus, block_ref, sems, kept,
):
    load = pltpu.make_async_copy(scaled_hbm.at[: scaled_ref.shape[0]], scaled_ref, kept)
    load.start()
    table_factors(factor_ref, plus.shape[0], plus, minus)
    load.wait()
    transform(core_ref[0], scaled_ref, factor_ref, plus, minus, block_ref, table_ref, sems, own_ref)


def chip_of(place_ref, h):
    across, along = place_ref[0] // 8, place_ref[0] // 2 % 4
    return ((across + h // 4) % 2) * 4 + (along + h % 4) % 4


def spread_rows(place_ref, factor_ref, out_ref):
    core = place_ref[0] % 2
    rows = out_ref.shape[1] // 4
    first = factor_ref.shape[0] - 2 * rows - 32
    inner_p = factor_ref[first : first + rows, :]
    inner_m = factor_ref[first + rows : first + 2 * rows, :]
    plus, minus = [], []
    for q in range(2):
        slab = chip_of(place_ref, 0) * 2 + (core + q) % 2
        c = jnp.broadcast_to(lead_of(factor_ref, 0, slab)[None], (rows // 16, 16, TILE)).reshape(rows, TILE)
        s = jnp.broadcast_to(lead_of(factor_ref, 1, slab)[None], (rows // 16, 16, TILE)).reshape(rows, TILE)
        plus.append(c * inner_p + s * inner_m)
        minus.append(c * inner_m - s * inner_p)
    left = lax.broadcasted_iota(jnp.int32, (rows, TILE), 1) < rows
    plus = jnp.where(left, plus[0], plus[1])
    minus = jnp.where(left, minus[0], minus[1])
    nothing = jnp.zeros((rows, TILE), BF16)
    for h in range(out_ref.shape[0]):
        for r in range(2):
            slab = chip_of(place_ref, h) * 2 + (core + r) % 2
            c = factor_ref[pl.ds(first + 2 * rows + slab, 1), :]
            s = factor_ref[pl.ds(first + 2 * rows + 16 + slab, 1), :]
            entry = (c * plus + s * minus).astype(BF16)
            for l in range(2):
                at = slice((2 * l + r) * rows, (2 * l + r + 1) * rows)
                out_ref[h, at, l * TILE : (l + 1) * TILE] = entry
                out_ref[h, at, (1 - l) * TILE : (2 - l) * TILE] = nothing


def pert_of(blocks, at):
    return jnp.concatenate([ref[:, at].reshape(-1, TILE) for ref in blocks], axis=0).astype(F32)


def cells(place_ref, *refs):
    blocks, (own_hbm, par_hbm, rows_ref, cells_hbm, turned_hbm) = refs[:8], refs[8:13]
    own, par, spread, cells_ref, turned_ref, reads, writes = refs[13:]
    members, depth, _ = own.shape
    rows = depth // 2
    last = blocks[0].shape[1] - 1
    loads = [
        pltpu.make_async_copy(own_hbm, own, reads.at[0]),
        pltpu.make_async_copy(par_hbm, par, reads.at[1]),
    ]
    for load in loads:
        load.start()
    lane = lax.broadcasted_iota(jnp.int32, (1, 2 * TILE), 1)
    row = lax.broadcasted_iota(jnp.int32, (4 * rows, 2 * TILE), 0)
    for h, block in enumerate(blocks):
        place = jnp.concatenate(
            [block[r, last].astype(F32)[0:1, :] for r in range(2)], axis=1
        ).astype(jnp.int32)
        level, inside = place // rows, place % rows
        place = level * (2 * rows) + inside + jnp.where(lane < TILE, 0, rows)
        chosen = (row == place).astype(F32).astype(BF16)
        spread[h] = lax.dot_general(
            chosen, rows_ref[h], (((0,), (0,)), ((), ())), preferred_element_type=F32
        ).astype(BF16)
    for load in loads:
        load.wait()
    stores = []
    for k in range(8):
        cols = slice(k * TILE, (k + 1) * TILE)
        along = jnp.concatenate(
            [
                jnp.concatenate(
                    [ref[m, l * rows : (l + 1) * rows, cols] for m in range(members)], axis=1
                )
                for l in range(2)
                for ref in (own, par)
            ],
            axis=0,
        )
        tiles = jnp.concatenate(
            [
                spread[h, r * TILE + k * 16 : r * TILE + (k + 1) * 16, :]
                for h in range(8)
                for r in range(2)
            ],
            axis=0,
        )
        field = jnp.dot(tiles, along, preferred_element_type=F32)
        total = None
        for m in range(members):
            term = pert_of(blocks, k * members + m) * field[:, m * TILE : (m + 1) * TILE]
            total = term if total is None else total + term
        total = total.astype(BF16)
        for h in range(8):
            cells_ref[k, chip_of(place_ref, h)] = total[h * 32 : (h + 1) * 32]
        stores.append(pltpu.make_async_copy(cells_ref.at[k], cells_hbm.at[k], writes.at[k]))
        stores[-1].start()
        turned = jnp.transpose(tiles.astype(F32)).astype(BF16)
        for q in range(2):
            for l in range(2):
                at = (2 * l + q) * rows
                turned_ref[k, (2 * q + l) * rows : (2 * q + l + 1) * rows, :] = turned[at : at + rows]
    stores.append(pltpu.make_async_copy(turned_ref, turned_hbm.at[:8], writes.at[8]))
    stores[-1].start()
    for store in stores:
        store.wait()


def score(cells_ref, own_ref, lent_ref, out_ref):
    copies = out_ref.shape[0]
    total = jnp.sum(cells_ref[...].astype(F32), axis=0)
    value = jnp.concatenate([own_ref[0], lent_ref[0]], axis=0)
    seen = jnp.concatenate([own_ref[1], lent_ref[1]], axis=0)
    resid = total - value
    result = jnp.where(seen > 0.5, resid / jnp.sqrt(1.0 + resid * resid * 0.25), 0.0)
    result = result.astype(BF16)
    for i in range(copies):
        out_ref[i] = result


def back(place_ref, *refs):
    blocks, (score_ref, turned_hbm, own_ref, par_ref, turned, sem) = refs[:8], refs[8:]
    members, depth, _ = own_ref.shape
    load = pltpu.make_async_copy(turned_hbm.at[:8], turned, sem)
    load.start()
    for k in range(8):
        weight = jnp.concatenate(
            [score_ref[k, chip_of(place_ref, h)] for h in range(8)], axis=0
        ).astype(F32)
        weighted = jnp.concatenate(
            [(pert_of(blocks, k * members + m) * weight).astype(BF16) for m in range(members)],
            axis=1,
        )
        if k == 0:
            load.wait()
        result = jnp.dot(turned[k], weighted, preferred_element_type=F32).astype(BF16)
        for m in range(members):
            part = result[:, m * TILE : (m + 1) * TILE]
            own_ref[m, :, k * TILE : (k + 1) * TILE] = part[:depth]
            par_ref[m, :, k * TILE : (k + 1) * TILE] = part[depth:]


def streamed(tables, rows, block_ref, sems):
    steps = tables[0].shape[0]

    def fetch(table, n, at):
        return pltpu.make_async_copy(table.at[n, rows, :], block_ref.at[at], sems.at[at])

    for n in range(3):
        fetch(tables[0], n, n).start()

    def block(n):
        @pl.when(n + 3 < steps)
        def _():
            fetch(tables[0], n + 3, n + 3).start()

        @pl.when((n + 3 >= steps) & (n + 3 < 2 * steps))
        def _():
            fetch(tables[1], n + 3 - steps, n + 3).start()

        fetch(tables[0], 0, n).wait()
        return block_ref[n]

    return block


def inverse_own(core_ref, own_ref, table0_ref, table1_ref, sum_ref, block_ref, sems):
    members, depth, width = own_ref.shape
    near = pl.ds(pl.multiple_of(core_ref[0] * width, width), width)
    block = streamed((table0_ref, table1_ref), near, block_ref, sems)

    def step(n, carry):
        sum_ref[n] = jnp.dot(
            own_ref[...].reshape(members * depth, width), block(n), preferred_element_type=F32
        )
        return carry

    lax.fori_loop(0, sum_ref.shape[0], step, 0)


def inverse_par(
    core_ref, par_ref, sum_ref, table0_ref, table1_ref, row_ref, col_ref, out_ref,
    piece, sems, block_ref, reads,
):
    members, depth, width = par_ref.shape
    levels, rows, _ = row_ref.shape
    core = core_ref[0]
    steps = sum_ref.shape[0]
    half = steps // 2
    far = pl.ds(pl.multiple_of((1 - core) * width, width), width)
    block = streamed((table0_ref, table1_ref), far, block_ref, reads)

    def copy(nb, slot):
        cols = pl.ds(pl.multiple_of(nb * WIDE, WIDE), WIDE)
        return pltpu.make_async_copy(piece.at[slot], out_ref.at[:, :, :, cols], sems.at[slot])

    def step(n, carry):
        slot = lax.rem(n, 2)
        nb = lax.rem(n + (1 - core) * half, steps)
        cols = pl.ds(pl.multiple_of(nb * WIDE, WIDE), WIDE)
        product = sum_ref[n] + jnp.dot(
            par_ref[...].reshape(members * depth, width), block(n), preferred_element_type=F32
        )
        product = product.reshape(members, levels, rows, WIDE)

        @pl.when(n >= 2)
        def _():
            copy(nb, slot).wait()

        for l in range(levels):
            amplitude = row_ref[l][:, :1] * col_ref[l : l + 1, cols]
            for m in range(members):
                piece[slot, m, l] = product[m, l] * amplitude
        copy(nb, slot).start()
        return carry

    lax.fori_loop(0, steps, step, 0)
    for slot in range(2):
        copy(slot, slot).wait()


def shards(control, perturbation, loc_row, loc_col, obs_tile, obs_count, obs_value):
    members, levels, rows, width = control.shape
    slabs = 16
    peers = lax.axis_size("member") * 8
    height = rows * slabs
    half = width // 2
    per_core = half // TILE
    depth = levels * rows
    across = lax.axis_index("across").astype(jnp.int32)
    along = lax.axis_index("along").astype(jnp.int32)
    core = lax.axis_index("core").astype(jnp.int32)
    group = lax.axis_index("member").astype(jnp.int32)
    core_index = core.reshape(1)
    place = (across * 8 + along * 2 + core).reshape(1)
    swap = [(0, 1), (1, 0)]

    def from_next(array, step):
        return lax.ppermute(array, "along", [((i + step) % 4, i) for i in range(4)])

    blocks = per_core * members + 1
    own_tiles, send_tiles = run(
        select,
        [bf16(blocks, 16, TILE)] * 2,
        [SMEM, HBM, HBM],
        1 << 27,
        [
            pltpu.VMEM((2, TILE), jnp.int32),
            pltpu.VMEM(perturbation.shape, BF16),
            pltpu.SemaphoreType.DMA((members + 1,)),
        ],
    )(core_index, obs_tile.reshape(2, TILE), perturbation)
    here = jnp.stack([own_tiles, lax.ppermute(send_tiles, "core", swap)])
    facing = lax.ppermute(here, "across", swap)
    here2 = from_next(here, 2)
    here1, here3 = from_next(here, 1), from_next(here, 3)
    facing1, facing3 = from_next(facing, 1), from_next(facing, 3)
    facing2 = lax.ppermute(here2, "across", swap)
    arrived = (here, here1, here2, here3, facing, facing1, facing2, facing3)

    lane = jnp.arange(TILE, dtype=jnp.int32)

    def of_column(column, array):
        return lax.dynamic_slice_in_dim(array, column * 16, 16, 0)

    seen = (lane[None, :] < obs_count[:, None]).astype(F32)
    mine = per_core * core + group
    other = per_core * (1 - core) + group
    stated = jnp.stack([of_column(mine, obs_value), of_column(mine, seen)])
    lent = jnp.stack([of_column(other, obs_value), of_column(other, seen)])
    lent = lax.ppermute(lent, "core", swap)

    lead = cas(np.arange(16), np.arange(16), 16)
    lead = np.repeat(np.stack(lead[2:]).reshape(-1, 1), TILE, axis=1)
    inner = 64
    outer = cas(np.arange(width // inner), np.arange(TILE), width // inner)
    near = cas(np.arange(inner), np.arange(TILE), width)
    root = np.float32(np.sqrt(width))
    factors = [outer[2], outer[3], near[0] / root, near[1] / root, lead]
    wave = np.arange(TILE) % rows
    base = cas(np.arange(rows), wave, height)
    turn = cas(np.arange(16), wave, 16)
    root = np.float32(np.sqrt(height))
    factors += [base[0] / root, base[1] / root, turn[2], turn[3]]
    factors = jnp.asarray(np.concatenate(factors))

    row_b = jnp.broadcast_to(loc_row[:, :, None], (levels, rows, TILE))
    table_half = bf16(width // WIDE // 2, width, WIDE)
    work = [
        pltpu.VMEM((members * depth, width), BF16),
        pltpu.VMEM((width, TILE), F32),
        pltpu.VMEM((width, TILE), F32),
        pltpu.VMEM((2, width, WIDE), BF16),
        pltpu.SemaphoreType.DMA((2,)),
    ]
    flops = members * depth * width * width
    send, scaled, table0 = run(
        forward_send,
        [bf16(members, depth, half), bf16(6 * members * depth, width), table_half],
        [SMEM, HBM, VMEM, VMEM, VMEM, HBM],
        flops,
        [pltpu.VMEM(control.shape, F32)]
        + work
        + [pltpu.SemaphoreType.DMA((members,)), pltpu.SemaphoreType.DMA],
        [VMEM, HBM, HBM],
        mib=50,
    )(core_index, control, row_b, loc_col, factors, here)
    par = lax.ppermute(send, "core", swap)
    own, table1 = run(
        forward_own,
        [bf16(members, depth, half), table_half],
        [SMEM, HBM, VMEM, HBM, HBM],
        flops,
        work + [pltpu.SemaphoreType.DMA],
        [VMEM, HBM],
        mib=50,
    )(core_index, scaled, factors, facing, here2)
    table_rows = run(
        spread_rows, bf16(8, 4 * rows, 2 * TILE), [SMEM, VMEM], 1 << 22
    )(place, factors)

    tiles = slabs * 16
    partial, turned = run(
        cells,
        [bf16(per_core, 8, 2 * 16, TILE), bf16(12 * per_core, 4 * rows, tiles)],
        [SMEM] + [VMEM] * 8 + [HBM, HBM, VMEM],
        1 << 30,
        [
            pltpu.VMEM((members, depth, half), BF16),
            pltpu.VMEM((members, depth, half), BF16),
            pltpu.VMEM((8, tiles, 4 * rows), BF16),
            pltpu.VMEM((per_core, 8, 2 * 16, TILE), BF16),
            pltpu.VMEM((per_core, 4 * rows, tiles), BF16),
            pltpu.SemaphoreType.DMA((2,)),
            pltpu.SemaphoreType.DMA((9,)),
        ],
        [HBM, HBM],
    )(place, *arrived, own, par, table_rows)
    partial = lax.all_to_all(
        partial.reshape(peers, 2 * 16, TILE), SAME_CORE, split_axis=0, concat_axis=0, tiled=True
    )
    scores = run(score, bf16(peers, 2 * 16, TILE), [VMEM] * 3, 1 << 20)(partial, stated, lent)
    scores = lax.all_to_all(scores, SAME_CORE, split_axis=0, concat_axis=0, tiled=True)

    back_own, back_send = run(
        back,
        [bf16(members, depth, half)] * 2,
        [SMEM] + [VMEM] * 9 + [HBM],
        1 << 28,
        [pltpu.VMEM((per_core, 4 * rows, tiles), BF16), pltpu.SemaphoreType.DMA],
        mib=46,
    )(place, *arrived, scores.reshape(per_core, 8, 2 * 16, TILE), turned)
    back_other = lax.ppermute(back_send, "core", swap)
    parts = width // WIDE
    stream = [pltpu.VMEM((parts, half, WIDE), BF16), pltpu.SemaphoreType.DMA((parts,))]
    summed = run(
        inverse_own,
        f32(width // WIDE, members * depth, WIDE),
        [SMEM, VMEM, HBM, HBM],
        flops,
        stream,
        mib=46,
    )(core_index, back_own, table0, table1)
    return run(
        inverse_par,
        f32(*control.shape),
        [SMEM, VMEM, VMEM, HBM, HBM, VMEM, VMEM],
        flops,
        [pltpu.VMEM((2, members, levels, rows, WIDE), F32), pltpu.SemaphoreType.DMA((2,))] + stream,
        [HBM],
        mib=46,
    )(core_index, back_other, summed, table0, table1, row_b, loc_col)


def solution(mesh):
    torus = Mesh(
        mesh.devices.reshape(mesh.shape["member"], 2, 4, 2),
        ("member", "across", "along", "core"),
    )
    placed = (
        P("member", None, SLAB, None),
        P("member", None, SLAB, None),
        P(None, SLAB),
        P(),
        P(SLAB),
        P(SLAB),
        P(SLAB, None),
    )
    return jax.shard_map(
        shards,
        mesh=torus,
        in_specs=placed,
        out_specs=P("member", None, SLAB, None),
        check_vma=False,
    )
```
